32 devices in a mesh: dp: 8 (over y, x, core), expert: 4 (over z).
Axes of the slice: x: 2, y: 2, z: 4, core: 2. Of those that a mesh axis runs over, the one named last changes fastest.
Arguments:
- out_grad: bfloat16 [64, 4096], P(('dp', 'expert')), may hold values from -0.29882812 to 0.29882812
- routes: int32 [64, 2], P('dp'), may hold values from 0 to 7, all different within a row; in each aligned block of 8 rows (0 to 7, 8 to 15, ...) at most 3 rows name the same one
- gate_values: bfloat16 [64, 2], P(('dp', 'expert')), may hold values from 0.099609375 to 1
- gate_pre: bfloat16 [8, 24, 12288], P('expert', None, 'dp'), may hold values from -6 to 6
- up_pre: bfloat16 [8, 24, 12288], P('expert', None, 'dp'), may hold values from -6 to 6
- w_down: bfloat16 [8, 12288, 4096], P('expert', 'dp'), may hold values from -0.0546875 to 0.0546875
Outputs:
- grad_gates: float32 [64, 2], P(('dp', 'expert'))
- grad_gate_pre: bfloat16 [8, 24, 12288], P('expert', None, 'dp')
- grad_up_pre: bfloat16 [8, 24, 12288], P('expert', None, 'dp')
- grad_down: bfloat16 [8, 12288, 4096], P('expert', 'dp')
The draws below stay inside these ranges and needn't reach their ends.
Inputs may be any that keep to these rules, and one draw needn't show every extreme that they name: `routes`: each token names two different experts. Among the 8 tokens of one block (aligned blocks of tokens, one for each dp index) no expert is named more than 3 times, and some expert reaches 3 in some block.
All inputs are finite; a program needn't handle non-finite values.
Results may differ from the reference program's by a relative error of at most 0.0049.
Values may be sent and summed in bfloat16 or wider, within the bound.
A program may use at most 128 MiB of HBM per device.

```python
import math
import jax
import jax.numpy as jnp
import numpy as np
from jax import lax

D = 4096
FF = 12288
EXPERTS = 8
TOK_DEV = 2
SLOTS = 3
TOKENS = 64
N_DP = 8
N_EXPERT = 4


def shard_levels(own_key, extent, split, smallest, high):
    level, own = 1.0, jax.random.fold_in(own_key, 6)
    for axis_at, parts in split:
        draws = jnp.exp(jax.random.uniform(jax.random.fold_in(own, axis_at), (parts,), jnp.float32, smallest / len(split), high / len(split)))
        level = level * jnp.repeat(draws, extent[axis_at] // parts).reshape([-1 if axis == axis_at else 1 for axis in range(len(extent))])
    return level


def routed_block(key, own, number, rows, number_of, top, bound, lean):
    sequence = jax.random.permutation(key, number_of)
    crowded, common = shares(number_of, rows * top, bound, lean, True), shares(number_of, rows * top, bound, lean, False)
    places = jnp.arange(number_of)

    def named(lengths, turn):
        used = int((lengths > 0).sum())
        fixed = max(1, used // 4)
        passed = fixed + (places - fixed + turn * (used - fixed)) % max(1, number_of - fixed)
        return jnp.zeros((number_of,), jnp.int32).at[sequence[jnp.where(places < fixed, places, passed)]].set(jnp.asarray(lengths, jnp.int32))

    lengths = jnp.where(number % 4 == 0, named(crowded, number // 4), named(common, number - number // 4 - 1))
    mixed = jax.random.permutation(jax.random.fold_in(own, 3), number_of)
    donor, receiver = mixed[0:number_of // 2 * 2:2], mixed[1:number_of // 2 * 2:2]
    room = jnp.minimum(lengths[donor] - 1, bound - lengths[receiver]) // 2
    room = jnp.where((donor == sequence[0]) | (receiver == sequence[0]) | (lengths[receiver] == 0), 0, jnp.maximum(room, 0))
    passed = jax.random.randint(jax.random.fold_in(own, 4), (number_of // 2,), 0, 1 << 20) % (room + 1)
    lengths = lengths.at[donor].add(-passed).at[receiver].add(passed)
    items = jnp.searchsorted(jnp.cumsum(lengths), jnp.arange(rows * top), side="right").astype(jnp.int32)
    listing = items.reshape(top, rows).T
    listing = listing[jax.random.permutation(jax.random.fold_in(own, 1), rows)]
    turn = jax.random.randint(jax.random.fold_in(own, 2), (rows, 1), 0, top)
    return jnp.take_along_axis(listing, (jnp.arange(top)[None, :] + turn) % top, axis=1)


def shares(count, total, limit, lean, full):
    loads = [(1 << 20) // math.isqrt(rank ** lean) + 1 for rank in range(1, count + 1)]
    largest = limit if full else min(limit, max(-(-total // count), total * loads[0] // sum(loads)))
    least = 1 if total - largest >= count - 1 else 0
    holding, surplus = [largest] + [least] * (count - 1), total - largest - least * (count - 1)
    while surplus > 0:
        movable = [i for i in range(1, count) if holding[i] < largest] or [i for i in range(1, count) if holding[i] < limit]
        whole, budget = sum([loads[i] for i in movable]), surplus
        for i in movable:
            extra = min(limit - holding[i], max(1, budget * loads[i] // whole), surplus)
            holding[i] = holding[i] + extra
            surplus = surplus - extra
    return np.array(holding)


def noise(own_key, shape, scale, limit, pieces=(), kind=jnp.bfloat16):
    drawn = scale * jax.random.normal(own_key, shape, jnp.float32)
    if pieces:
        drawn = drawn * shard_levels(own_key, shape, pieces, -0.22, 0.18)
    return jnp.clip(drawn, -limit, limit).astype(kind)


def setup_inputs(seed: int = 0) -> dict:
    streams_of = jax.random.split(jax.random.key(seed), 7)
    out_grad = noise(streams_of[0], (TOKENS, D), 0.05, 0.29882812, ((0, 32),))
    routes_keys = jax.random.split(jax.random.fold_in(streams_of[1], 1), TOKENS // (N_EXPERT * TOK_DEV))
    routes_turns = jax.random.permutation(jax.random.fold_in(streams_of[1], 3), TOKENS // (N_EXPERT * TOK_DEV))
    routes = jax.vmap(lambda own, number: routed_block(jax.random.fold_in(streams_of[1], 2), own, number, N_EXPERT * TOK_DEV, EXPERTS, 2, SLOTS, 1))(routes_keys, routes_turns).reshape((TOKENS, 2))
    gate_values = jnp.clip(0.099609375 + 0.9003906 * jax.random.uniform(streams_of[2], (TOKENS, 2), jnp.float32) ** shard_levels(streams_of[2], (TOKENS, 2), ((0, 32),), -0.2, 0.2), 0.099609375, 1.0).astype(jnp.bfloat16)
    gate_pre = noise(streams_of[3], (EXPERTS, N_DP * SLOTS, FF), 1.0, 6.0, ((0, 4), (2, 8)))
    up_pre = noise(streams_of[4], (EXPERTS, N_DP * SLOTS, FF), 1.0, 6.0, ((0, 4), (2, 8)))
    w_down = noise(streams_of[5], (EXPERTS, FF, D), FF ** -0.5, 0.0546875, ((0, 4), (1, 8)))
    return {"out_grad": out_grad, "routes": routes, "gate_values": gate_values, "gate_pre": gate_pre, "up_pre": up_pre, "w_down": w_down}


def slot_rows(routes):
    flat_routes = routes.reshape(N_DP, -1)
    onehot = (flat_routes[:, :, None] == jnp.arange(EXPERTS, dtype=jnp.int32)[None, None, :]).astype(jnp.int32)
    position = jnp.sum((jnp.cumsum(onehot, axis=1) - 1) * onehot, axis=2)
    slot_row = jnp.arange(N_DP, dtype=jnp.int32)[:, None] * SLOTS + position
    return slot_row.reshape(-1).astype(jnp.int32)


def reference(out_grad, routes, gate_values, gate_pre, up_pre, w_down):
    expert = routes.reshape(-1).astype(jnp.int32)
    slot_row = slot_rows(routes)
    token_index = jnp.repeat(jnp.arange(TOKENS, dtype=jnp.int32), 2)
    dispatched = jnp.zeros((EXPERTS, N_DP * SLOTS, D), jnp.bfloat16).at[expert, slot_row].set(out_grad[token_index])
    slot_gate = jnp.zeros((EXPERTS, N_DP * SLOTS), jnp.bfloat16).at[expert, slot_row].set(gate_values.reshape(-1))

    def per_expert(packed):
        gate_block, up_block, weights, rows_in, gate_row = packed
        projected = jnp.dot(rows_in, weights.T, preferred_element_type=jnp.float32)
        gate_act = gate_block.astype(jnp.float32)
        up_act = up_block.astype(jnp.float32)
        sigmoid_val = jax.nn.sigmoid(gate_act)
        silu_val = gate_act * sigmoid_val
        hidden = silu_val * up_act
        partial_value = jnp.sum(hidden * projected, axis=1)
        scale_col = gate_row.astype(jnp.float32)[:, None]
        weighted = (scale_col * hidden).astype(jnp.bfloat16)
        down_grad = jnp.dot(weighted.T, rows_in, preferred_element_type=jnp.float32).astype(jnp.bfloat16)
        grad_hidden = scale_col * projected
        grad_gate = (grad_hidden * up_act * sigmoid_val * (1.0 + gate_act * (1.0 - sigmoid_val))).astype(jnp.bfloat16)
        grad_up = (grad_hidden * silu_val).astype(jnp.bfloat16)
        return partial_value, grad_gate, grad_up, down_grad

    partial_value, grad_gate_pre, grad_up_pre, grad_down = lax.map(per_expert, (gate_pre, up_pre, w_down, dispatched, slot_gate))
    grad_gates = partial_value[expert, slot_row].reshape(TOKENS, 2)
    return grad_gates, grad_gate_pre, grad_up_pre, grad_down
```

```python
import functools

import jax
import jax.numpy as jnp
from jax import lax
from jax.experimental import pallas as pl
from jax.experimental.pallas import tpu as pltpu
from jax.sharding import PartitionSpec as P

SLOTS = 3


def expert_terms(gate_piece, up_piece, weights, rows_in, gate_row):
    projected = jnp.einsum("erd,efd->erf", rows_in, weights, preferred_element_type=jnp.float32)
    gate_act = gate_piece.astype(jnp.float32)
    up_act = up_piece.astype(jnp.float32)
    sigmoid_val = jax.nn.sigmoid(gate_act)
    silu_val = gate_act * sigmoid_val
    hidden = silu_val * up_act
    partial_value = jnp.sum(hidden * projected, axis=2)
    scale_col = gate_row.astype(jnp.float32)[:, :, None]
    weighted = (scale_col * hidden).astype(jnp.bfloat16)
    down_term = jnp.einsum("erf,erd->efd", weighted, rows_in, preferred_element_type=jnp.float32)
    grad_hidden = scale_col * projected
    grad_gate = (
        grad_hidden * up_act * sigmoid_val * (1.0 + gate_act * (1.0 - sigmoid_val))
    ).astype(jnp.bfloat16)
    grad_up = (grad_hidden * silu_val).astype(jnp.bfloat16)
    return (partial_value, grad_gate, grad_up, down_term)


def general_device(out_grad, routes, gate_values, gate_pre, up_pre, w_down):
    groups = lax.axis_size("expert")
    local_count = gate_pre.shape[0]
    experts = local_count * groups
    tok_count = out_grad.shape[0]
    my_rank = lax.axis_index("expert")
    flat_routes = routes.reshape(-1)
    onehot = (flat_routes[:, None] == jnp.arange(experts, dtype=jnp.int32)[None, :]).astype(
        jnp.int32
    )
    position = jnp.sum((jnp.cumsum(onehot, axis=0) - 1) * onehot, axis=1)
    own_expert = lax.dynamic_slice_in_dim(flat_routes, my_rank * tok_count * 2, tok_count * 2)
    own_position = lax.dynamic_slice_in_dim(position, my_rank * tok_count * 2, tok_count * 2)
    target = own_expert * SLOTS + own_position
    selector = target[:, None] == jnp.arange(experts * SLOTS, dtype=jnp.int32)[None, :]
    picker = selector.astype(jnp.bfloat16).T
    pair_rows = jnp.repeat(out_grad, 2, axis=0)
    send_rows = (
        jnp.dot(picker, pair_rows, preferred_element_type=jnp.float32)
        .astype(jnp.bfloat16)
        .reshape(experts, SLOTS, -1)
    )
    send_gates = (
        jnp.dot(picker, gate_values.reshape(-1, 1), preferred_element_type=jnp.float32)
        .astype(jnp.bfloat16)
        .reshape(experts, SLOTS)
    )
    got_rows, got_gates = (
        lax.all_to_all(send_rows, "expert", split_axis=0, concat_axis=0, tiled=True),
        lax.all_to_all(send_gates, "expert", split_axis=0, concat_axis=0, tiled=True),
    )
    dispatched = jnp.sum(
        got_rows.reshape(groups, local_count, SLOTS, -1).astype(jnp.float32), axis=0
    ).astype(jnp.bfloat16)
    slot_gate = jnp.sum(
        got_gates.reshape(groups, local_count, SLOTS).astype(jnp.float32), axis=0
    ).astype(jnp.bfloat16)
    all_rows, all_gates = (
        lax.all_gather(dispatched, "dp", axis=1, tiled=True),
        lax.all_gather(slot_gate, "dp", axis=1, tiled=True),
    )
    partial_value, grad_gate_pre, grad_up_pre, down_sum = expert_terms(
        gate_pre, up_pre, w_down, all_rows, all_gates
    )
    grad_down = down_sum.astype(jnp.bfloat16)
    own_sums = lax.psum_scatter(partial_value, "dp", scatter_dimension=1, tiled=True)
    score_table = lax.all_gather(own_sums, "expert", axis=0, tiled=True)
    picked = jnp.sum(jnp.where(selector, score_table.reshape(1, -1), 0.0), axis=1)
    grad_gates = picked.reshape(tok_count, 2)
    return (grad_gates, grad_gate_pre, grad_up_pre, grad_down)


LANES = 128
CORES = 2
PAD = 4
MESH = pl.DeviceIdType.MESH
BF16 = jnp.bfloat16
F32 = jnp.float32


def fused_fits(n_dp, groups, tokens, width, local, rows, hidden):
    return (
        n_dp % CORES == 0
        and n_dp > CORES
        and groups > 1
        and local * PAD == 8
        and rows == n_dp * SLOTS
        and n_dp * 8 <= LANES
        and groups * tokens <= LANES
        and width % (4 * LANES) == 0
        and hidden % 512 == 0
        and n_dp * groups <= 64
        and local * hidden * width * 2 <= 26 << 20
    )


def gather_project(
    n_dp, groups, local, rows, block, pieces, early,
    grad, routes, gates, gate_pre, up_pre, weights,
    rows_out, turned_out, grad_gate_out, grad_up_out, sums_out,
    held, tokens_in, gates_in, routes_in, gate_in, up_in,
    table, picked, high, totals, silu_kept, slope_kept, turned_kept,
    sums_own, sums_all,
    load_sem, in_sem, send_z, recv_z, send_g, recv_g, send_c, recv_c, send_p, recv_p,
    send_s, recv_s,
):
    me_dp, me_z = lax.axis_index("dp"), lax.axis_index("expert")
    total = n_dp * groups
    me = me_dp * groups + me_z
    chips = n_dp // CORES
    chip, core = me_dp // CORES, lax.rem(me_dp, CORES)
    partner = chip * CORES + (1 - core)
    tokens, width = grad.shape
    hidden = held.shape[1]
    per = hidden // block
    steps = local * per
    half = width // 2
    full = n_dp * 8
    span = tokens * groups

    barrier = pltpu.get_barrier_semaphore()
    peers = [(me_dp, lax.rem(me_z + dz, groups)) for dz in range(1, groups)]
    peers += [(lax.rem(chip + dc, chips) * CORES + core, me_z) for dc in range(1, chips)]
    peers += [(partner, me_z)]
    for peer in peers:
        pl.semaphore_signal(barrier, inc=1, device_id=peer, device_id_type=MESH)

    def local_copy(src, dst, at):
        copy = pltpu.make_async_copy(src, dst, in_sem.at[at])
        copy.start()
        return copy

    own_rows = local_copy(grad, tokens_in.at[me_z], 0)
    own_gates = local_copy(gates, gates_in.at[me_z], 1)
    own_routes = local_copy(routes, routes_in, 2)
    own_pre = local_copy(gate_pre, gate_in, 3)
    own_up = local_copy(up_pre, up_in, 4)

    def weight_copy(i):
        e, b = i // per, lax.rem(i, per)
        where = pl.ds(b * block, block)
        return pltpu.make_async_copy(weights.at[e, where], held.at[e, where], load_sem.at[i])

    for i in range(steps):
        weight_copy(i).start()

    own_routes.wait()
    first, second = routes_in[0:1, :], routes_in[1:2, :]
    row8 = lax.broadcasted_iota(jnp.int32, (8, 1), 0)
    lane8 = lax.broadcasted_iota(jnp.int32, (1, span), 1)
    expert_of = me_z * local + row8 // PAD
    slot_of = lax.rem(row8, PAD)
    by_choice = [(route == expert_of) for route in (first, second)]
    named = jnp.where(by_choice[0] | by_choice[1], 1, 0)
    before = jnp.zeros((8, span), jnp.int32)
    for t in range(span - 1):
        before = before + jnp.where(lane8 > t, named[:, t : t + 1], 0)
    fills = (before == slot_of) & (named > 0)
    select = jnp.where(fills, 1.0, 0.0)
    select_by = [jnp.where(fills & choice, 1.0, 0.0) for choice in by_choice]

    own_rows.wait()
    own_gates.wait()
    pl.semaphore_wait(barrier, len(peers))
    stage_one = []
    for dz in range(1, groups):
        peer = (me_dp, lax.rem(me_z + dz, groups))
        for ref, s_sem, r_sem in ((tokens_in, send_z, recv_z), (gates_in, send_g, recv_g)):
            copy = pltpu.make_async_remote_copy(
                src_ref=ref.at[me_z], dst_ref=ref.at[me_z],
                send_sem=s_sem.at[dz], recv_sem=r_sem.at[dz],
                device_id=peer, device_id_type=MESH,
            )
            copy.start()
            stage_one.append(copy)

    own_pre.wait()
    own_up.wait()
    wide_row = lax.broadcasted_iota(jnp.int32, (full, 1), 0)
    pair_row = lax.broadcasted_iota(jnp.int32, (1, rows), 1)
    spot = (wide_row // 8) * SLOTS + lax.rem(wide_row, PAD)
    real = lax.rem(wide_row, PAD) < SLOTS
    spread = []
    for e in range(local):
        mine = real & (lax.rem(wide_row, 8) // PAD == e)
        spread.append(jnp.where(mine & (spot == pair_row), 1.0, 0.0))
    flip_row = lax.broadcasted_iota(jnp.int32, (rows, 1), 0)
    flip_col = lax.broadcasted_iota(jnp.int32, (1, full), 1)
    flip_spot = (flip_col // 8) * SLOTS + lax.rem(flip_col, PAD)
    flip_real = lax.rem(flip_col, PAD) < SLOTS
    unspread = []
    for e in range(local):
        mine = flip_real & (lax.rem(flip_col, 8) // PAD == e)
        unspread.append(jnp.where(mine & (flip_spot == flip_row), 1.0, 0.0).astype(BF16))

    owner = lax.rem(wide_row, 8) // PAD
    for c in range(0, hidden, 512):
        cols = slice(c, c + 512)
        gate_act = jnp.zeros((full, 512), F32)
        up_act = jnp.zeros((full, 512), F32)
        for e in range(local):
            pick = spread[e].astype(BF16)
            gate_act += jnp.dot(pick, gate_in[e, :, cols], preferred_element_type=F32)
            up_act += jnp.dot(pick, up_in[e, :, cols], preferred_element_type=F32)
        sigmoid_val = jax.nn.sigmoid(gate_act)
        silu_val = gate_act * sigmoid_val
        act = silu_val * up_act
        silu_kept[:, cols] = silu_val
        slope_kept[:, cols] = up_act * sigmoid_val * (1.0 + gate_act * (1.0 - sigmoid_val))
        turned_kept[cols, :] = act.T
        for e in range(local):
            part = jnp.where(owner == e, act, 0.0)
            top = part.astype(BF16)
            rest = (part - top.astype(F32)).astype(BF16)
            for b in range(512 // block):
                at = slice(b * block, (b + 1) * block)
                high[e * per + c // block + b, :full] = top[:, at]
                high[e * per + c // block + b, full:] = rest[:, at]

    def forward_step(i):
        e, b = i // per, lax.rem(i, per)
        weight_copy(i).wait()
        left = high[i]
        for n in range(0, width, 512):
            totals[:, n : n + 512] += jnp.dot(
                left,
                held[e, pl.ds(pl.multiple_of(b * block, block), block), n : n + 512],
                preferred_element_type=F32,
            )

    def forward_steps(low, top):
        def body(i, carry):
            forward_step(i)
            return carry

        lax.fori_loop(low, top, body, 0)

    totals[...] = jnp.zeros_like(totals)
    forward_steps(0, early[0])

    for copy in stage_one:
        copy.wait_recv()
    slots = jnp.zeros((8, width), F32)
    gate = jnp.zeros((8, 1), F32)
    for z in range(groups):
        got = tokens_in[z].astype(F32)
        got_gate = gates_in[z].astype(F32)
        for t in range(tokens):
            at = z * tokens + t
            slots = slots + select[:, at : at + 1] * got[t : t + 1, :]
            for k in range(2):
                gate = gate + select_by[k][:, at : at + 1] * got_gate[t : t + 1, k : k + 1]
    gate_wide = jnp.broadcast_to(gate, (8, LANES))
    base = pl.multiple_of(me_dp * 16, 16)
    table[pl.ds(base, 16), :half] = jnp.concatenate(
        [slots[:, :half], slots[:, half:]], axis=0
    ).astype(BF16)
    table[pl.ds(base, 16), half:] = jnp.concatenate([gate_wide, gate_wide], axis=0).astype(BF16)

    def block_copy(dp_index, target, piece, s_sem, r_sem):
        where = table.at[pl.ds(dp_index * 16, 16), pl.ds(pieces[piece], pieces[piece + 1] - pieces[piece])]
        copy = pltpu.make_async_remote_copy(
            src_ref=where, dst_ref=where, send_sem=s_sem, recv_sem=r_sem,
            device_id=(target, me_z), device_id_type=MESH,
        )
        copy.start()
        return copy

    count = len(pieces) - 1
    stage_two = {}
    stage_three = {}
    for p in range(count):
        for dc in range(1, chips):
            target = lax.rem(chip + dc, chips) * CORES + core
            stage_two[p, dc] = block_copy(me_dp, target, p, send_c.at[p, dc], recv_c.at[p, dc])
        stage_three[p, 0] = block_copy(me_dp, partner, p, send_p.at[p, 0], recv_p.at[p, 0])

    forward_steps(early[0], early[1])

    for p in range(count):
        for dc in range(1, chips):
            stage_two[p, dc].wait_recv()
            source = lax.rem(chip - dc + chips, chips) * CORES + core
            stage_three[p, dc] = block_copy(source, partner, p, send_p.at[p, dc], recv_p.at[p, dc])

    forward_steps(early[1], steps)

    for copy in stage_three.values():
        copy.wait_recv()

    part = jnp.zeros((full, LANES), F32)
    for h in range(2):
        for n in range(0, half, 512):
            got = table[:, n : n + 512].astype(F32).reshape(n_dp, 16, 512)
            got = got[:, h * 8 : h * 8 + 8].reshape(full, 512)
            at = slice(h * half + n, h * half + n + 512)
            picked[:, at] = got.astype(BF16)
            term = got * (totals[:full, at] + totals[full:, at])
            for q in range(0, 512, LANES):
                part = part + term[:, q : q + LANES]
    rows_out[...] = picked[...]
    part = jnp.sum(part, axis=1, keepdims=True)
    lane = lax.broadcasted_iota(jnp.int32, (full, LANES), 1)
    sums = jnp.sum(jnp.where(lane == wide_row, part, 0.0), axis=0, keepdims=True)
    sums_own[...] = sums
    sums_all[me] = sums
    last = []
    for off in range(1, total):
        other = lax.rem(me + off, total)
        copy = pltpu.make_async_remote_copy(
            src_ref=sums_own, dst_ref=sums_all.at[me],
            send_sem=send_s.at[off], recv_sem=recv_s.at[off],
            device_id=(other // groups, lax.rem(other, groups)), device_id_type=MESH,
        )
        copy.start()
        last.append(copy)

    scale = table[:, half:].astype(F32).reshape(n_dp, 16, LANES)[:, :8].reshape(full, LANES)
    scale_row = scale.T[0:1, :]
    scale_col = scale[:, 0:1]
    col = lax.broadcasted_iota(jnp.int32, (1, full), 1)
    for e in range(local):
        factor = jnp.where(lax.rem(col, 8) // PAD == e, scale_row, 0.0)
        turned_out[e] = (turned_kept[...] * factor).astype(BF16)
    for c in range(0, hidden, 512):
        cols = slice(c, c + 512)
        both = [
            lax.dot_general(
                picked[...], held[e, cols], (((1,), (1,)), ((), ())),
                preferred_element_type=F32,
            )
            for e in range(local)
        ]
        proj = both[0]
        for e in range(1, local):
            proj = jnp.where(owner == e, both[e], proj)
        grad_hidden = scale_col * proj
        gate_grad = (grad_hidden * slope_kept[:, cols]).astype(BF16)
        up_grad = (grad_hidden * silu_kept[:, cols]).astype(BF16)
        for e in range(local):
            for ref, value in ((grad_gate_out, gate_grad), (grad_up_out, up_grad)):
                ref[e, :, cols] = jnp.dot(
                    unspread[e], value, preferred_element_type=F32
                ).astype(BF16)

    for copy in last:
        copy.wait_recv()
    sums_by = []
    for z in range(groups):
        acc = sums_all[z]
        for d in range(1, n_dp):
            acc = acc + sums_all[d * groups + z]
        sums_by.append(acc)
    out_row = lax.broadcasted_iota(jnp.int32, sums_out.shape, 0)
    out_col = lax.broadcasted_iota(jnp.int32, sums_out.shape, 1)
    spots = lax.broadcasted_iota(jnp.int32, (1, LANES), 1)
    result = jnp.zeros(sums_out.shape, F32)
    for k, route in enumerate((first, second)):
        ahead = jnp.zeros((1, span), jnp.int32)
        for t in range(span - 1):
            same = (first[:, t : t + 1] == route) | (second[:, t : t + 1] == route)
            ahead = ahead + jnp.where((lane8 > t) & same, 1, 0)
        for t in range(tokens):
            here = lane8 == me_z * tokens + t
            expert = jnp.sum(jnp.where(here, route, 0), axis=1, keepdims=True)
            place = jnp.sum(jnp.where(here, ahead, 0), axis=1, keepdims=True)
            value = jnp.zeros((1, LANES), F32)
            for z in range(groups):
                offset = expert - z * local
                code = jnp.where(
                    (offset >= 0) & (offset < local), me_dp * 8 + offset * PAD + place, -1
                )
                value = value + jnp.where(spots == code, sums_by[z], 0.0)
            value = jnp.sum(value, axis=1, keepdims=True)
            result = jnp.where((out_row == t) & (out_col == k), value, result)
    sums_out[...] = result
    for copy in stage_one + list(stage_two.values()) + list(stage_three.values()) + last:
        copy.wait_send()


def finish(
    block, rows_in, turned, gate_grad, up_grad, sums,
    grad_sums, grad_gate, grad_up, grad_down, made, small_sem, out_sem,
):
    local, hidden, _ = turned.shape
    width = rows_in.shape[1]
    per = hidden // block
    small = []
    for at, (src, dst) in enumerate(
        ((sums, grad_sums), (gate_grad, grad_gate), (up_grad, grad_up))
    ):
        copy = pltpu.make_async_copy(src, dst, small_sem.at[at])
        copy.start()
        small.append(copy)

    def out_copy(i):
        e, b = i // per, lax.rem(i, per)
        where = pl.ds(b * block, block)
        return pltpu.make_async_copy(made.at[e, where], grad_down.at[e, where], out_sem.at[i])

    def body(i, carry):
        e, b = i // per, lax.rem(i, per)
        where = pl.ds(pl.multiple_of(b * block, block), block)
        left = turned[e, where, :]
        for n in range(0, width, 512):
            made[e, where, n : n + 512] = jnp.dot(
                left, rows_in[:, n : n + 512], preferred_element_type=F32
            ).astype(BF16)
        out_copy(i).start()
        return carry

    lax.fori_loop(0, local * per, body, 0)

    def drain(i, carry):
        out_copy(i).wait()
        return carry

    lax.fori_loop(0, local * per, drain, 0)
    for copy in small:
        copy.wait()


def fused_device(out_grad, routes, gate_values, gate_pre, up_pre, w_down):
    n_dp, groups = lax.axis_size("dp"), lax.axis_size("expert")
    tokens, width = out_grad.shape
    local, rows, hidden = gate_pre.shape
    block = 512
    total = n_dp * groups
    full = n_dp * 8
    half = width // 2
    chips = n_dp // CORES
    pieces = (0, half // 2, half + LANES)
    count = len(pieces) - 1
    steps = local * hidden // block
    early = (steps // 2, steps - 1)
    span = groups * tokens

    vmem = pl.BlockSpec(memory_space=pltpu.VMEM)
    hbm = pl.BlockSpec(memory_space=pltpu.HBM)
    dma = pltpu.SemaphoreType.DMA
    scratch = pltpu.VMEM
    rows_in, turned, gate_grad, up_grad, sums = pl.pallas_call(
        functools.partial(gather_project, n_dp, groups, local, rows, block, pieces, early),
        out_shape=(
            pltpu.VMEM((full, width), BF16),
            pltpu.VMEM((local, hidden, full), BF16),
            pltpu.VMEM(gate_pre.shape, BF16),
            pltpu.VMEM(up_pre.shape, BF16),
            pltpu.VMEM((tokens, 2), F32),
        ),
        in_specs=[hbm] * 6,
        out_specs=(vmem,) * 5,
        scratch_shapes=[
            scratch((local, hidden, width), BF16),
            scratch((groups, tokens, width), BF16),
            scratch((groups, tokens, 2), BF16),
            scratch((2, span), jnp.int32),
            scratch(gate_pre.shape, BF16),
            scratch(up_pre.shape, BF16),
            scratch((n_dp * 16, half + LANES), BF16),
            scratch((full, width), BF16),
            scratch((steps, 2 * full, block), BF16),
            scratch((2 * full, width), F32),
            scratch((full, hidden), F32),
            scratch((full, hidden), F32),
            scratch((hidden, full), F32),
            scratch((1, LANES), F32),
            scratch((total, 1, LANES), F32),
            dma((steps,)),
            dma((5,)),
            dma((groups,)),
            dma((groups,)),
            dma((groups,)),
            dma((groups,)),
            dma((count, chips)),
            dma((count, chips)),
            dma((count, chips)),
            dma((count, chips)),
            dma((total,)),
            dma((total,)),
        ],
        compiler_params=pltpu.CompilerParams(
            collective_id=0, has_side_effects=True, vmem_limit_bytes=52 << 20
        ),
        name="gather_project",
    )(out_grad, routes.T, gate_values, gate_pre, up_pre, w_down)

    piece = 256
    return pl.pallas_call(
        functools.partial(finish, piece),
        out_shape=(
            jax.ShapeDtypeStruct((tokens, 2), F32),
            jax.ShapeDtypeStruct(gate_pre.shape, BF16),
            jax.ShapeDtypeStruct(up_pre.shape, BF16),
            jax.ShapeDtypeStruct(w_down.shape, BF16),
        ),
        in_specs=[vmem] * 5,
        out_specs=(hbm,) * 4,
        scratch_shapes=[
            scratch((local, hidden, width), BF16),
            dma((3,)),
            dma((local * hidden // piece,)),
        ],
        compiler_params=pltpu.CompilerParams(vmem_limit_bytes=52 << 20),
        name="finish",
    )(rows_in, turned, gate_grad, up_grad, sums)


def per_device(out_grad, routes, gate_values, gate_pre, up_pre, w_down):
    fits = fused_fits(
        lax.axis_size("dp"), lax.axis_size("expert"), *out_grad.shape, *gate_pre.shape
    )
    chosen = fused_device if fits else general_device
    return chosen(out_grad, routes, gate_values, gate_pre, up_pre, w_down)


def solution(mesh):
    return jax.shard_map(
        per_device,
        mesh=mesh,
        in_specs=(
            P(("dp", "expert"), None),
            P("dp", None),
            P(("dp", "expert"), None),
            P("expert", None, "dp"),
            P("expert", None, "dp"),
            P("expert", "dp", None),
        ),
        out_specs=(
            P(("dp", "expert"), None),
            P("expert", None, "dp"),
            P("expert", None, "dp"),
            P("expert", "dp", None),
        ),
        check_vma=False,
    )
```

```python
import functools

import jax
import jax.numpy as jnp
from jax import lax
from jax.experimental import pallas as pl
from jax.experimental.pallas import tpu as pltpu
from jax.sharding import PartitionSpec as P

SLOTS = 3


def expert_terms(gate_piece, up_piece, weights, rows_in, gate_row):
    projected = jnp.einsum("erd,efd->erf", rows_in, weights, preferred_element_type=jnp.float32)
    gate_act = gate_piece.astype(jnp.float32)
    up_act = up_piece.astype(jnp.float32)
    sigmoid_val = jax.nn.sigmoid(gate_act)
    silu_val = gate_act * sigmoid_val
    hidden = silu_val * up_act
    partial_value = jnp.sum(hidden * projected, axis=2)
    scale_col = gate_row.astype(jnp.float32)[:, :, None]
    weighted = (scale_col * hidden).astype(jnp.bfloat16)
    down_term = jnp.einsum("erf,erd->efd", weighted, rows_in, preferred_element_type=jnp.float32)
    grad_hidden = scale_col * projected
    grad_gate = (
        grad_hidden * up_act * sigmoid_val * (1.0 + gate_act * (1.0 - sigmoid_val))
    ).astype(jnp.bfloat16)
    grad_up = (grad_hidden * silu_val).astype(jnp.bfloat16)
    return (partial_value, grad_gate, grad_up, down_term)


def general_device(out_grad, routes, gate_values, gate_pre, up_pre, w_down):
    groups = lax.axis_size("expert")
    local_count = gate_pre.shape[0]
    experts = local_count * groups
    tok_count = out_grad.shape[0]
    my_rank = lax.axis_index("expert")
    flat_routes = routes.reshape(-1)
    onehot = (flat_routes[:, None] == jnp.arange(experts, dtype=jnp.int32)[None, :]).astype(
        jnp.int32
    )
    position = jnp.sum((jnp.cumsum(onehot, axis=0) - 1) * onehot, axis=1)
    own_expert = lax.dynamic_slice_in_dim(flat_routes, my_rank * tok_count * 2, tok_count * 2)
    own_position = lax.dynamic_slice_in_dim(position, my_rank * tok_count * 2, tok_count * 2)
    target = own_expert * SLOTS + own_position
    selector = target[:, None] == jnp.arange(experts * SLOTS, dtype=jnp.int32)[None, :]
    picker = selector.astype(jnp.bfloat16).T
    pair_rows = jnp.repeat(out_grad, 2, axis=0)
    send_rows = (
        jnp.dot(picker, pair_rows, preferred_element_type=jnp.float32)
        .astype(jnp.bfloat16)
        .reshape(experts, SLOTS, -1)
    )
    send_gates = (
        jnp.dot(picker, gate_values.reshape(-1, 1), preferred_element_type=jnp.float32)
        .astype(jnp.bfloat16)
        .reshape(experts, SLOTS)
    )
    got_rows, got_gates = (
        lax.all_to_all(send_rows, "expert", split_axis=0, concat_axis=0, tiled=True),
        lax.all_to_all(send_gates, "expert", split_axis=0, concat_axis=0, tiled=True),
    )
    dispatched = jnp.sum(
        got_rows.reshape(groups, local_count, SLOTS, -1).astype(jnp.float32), axis=0
    ).astype(jnp.bfloat16)
    slot_gate = jnp.sum(
        got_gates.reshape(groups, local_count, SLOTS).astype(jnp.float32), axis=0
    ).astype(jnp.bfloat16)
    all_rows, all_gates = (
        lax.all_gather(dispatched, "dp", axis=1, tiled=True),
        lax.all_gather(slot_gate, "dp", axis=1, tiled=True),
    )
    partial_value, grad_gate_pre, grad_up_pre, down_sum = expert_terms(
        gate_pre, up_pre, w_down, all_rows, all_gates
    )
    grad_down = down_sum.astype(jnp.bfloat16)
    own_sums = lax.psum_scatter(partial_value, "dp", scatter_dimension=1, tiled=True)
    score_table = lax.all_gather(own_sums, "expert", axis=0, tiled=True)
    picked = jnp.sum(jnp.where(selector, score_table.reshape(1, -1), 0.0), axis=1)
    grad_gates = picked.reshape(tok_count, 2)
    return (grad_gates, grad_gate_pre, grad_up_pre, grad_down)


LANES = 128
CORES = 2
PAD = 4
MESH = pl.DeviceIdType.MESH
BF16 = jnp.bfloat16
F32 = jnp.float32


def fused_fits(n_dp, groups, tokens, width, local, rows, hidden):
    return (
        n_dp % CORES == 0
        and n_dp > CORES
        and groups > 1
        and local * PAD == 8
        and rows == n_dp * SLOTS
        and n_dp * 8 <= LANES
        and groups * tokens <= LANES
        and width % (4 * LANES) == 0
        and hidden % 512 == 0
        and n_dp * groups <= 64
        and local * hidden * width * 2 <= 26 << 20
    )


def gather_project(
    n_dp, groups, local, rows, block, pieces, early, flipped,
    grad, routes, gates, gate_pre, up_pre, weights,
    rows_out, turned_out, grad_gate_out, grad_up_out, sums_out,
    held, tokens_in, gates_in, routes_in, gate_in, up_in,
    table, picked, high, totals, flips, silu_kept, slope_kept, turned_kept,
    sums_own, sums_all,
    load_sem, in_sem, send_z, recv_z, send_g, recv_g, send_c, recv_c, send_p, recv_p,
    send_s, recv_s,
):
    me_dp, me_z = lax.axis_index("dp"), lax.axis_index("expert")
    total = n_dp * groups
    me = me_dp * groups + me_z
    chips = n_dp // CORES
    chip, core = me_dp // CORES, lax.rem(me_dp, CORES)
    partner = chip * CORES + (1 - core)
    tokens, width = grad.shape
    hidden = held.shape[1]
    per = hidden // block
    steps = local * per
    half = width // 2
    full = n_dp * 8
    span = tokens * groups

    barrier = pltpu.get_barrier_semaphore()
    peers = [(me_dp, lax.rem(me_z + dz, groups)) for dz in range(1, groups)]
    peers += [(lax.rem(chip + dc, chips) * CORES + core, me_z) for dc in range(1, chips)]
    peers += [(partner, me_z)]
    for peer in peers:
        pl.semaphore_signal(barrier, inc=1, device_id=peer, device_id_type=MESH)

    def local_copy(src, dst, at):
        copy = pltpu.make_async_copy(src, dst, in_sem.at[at])
        copy.start()
        return copy

    own_rows = local_copy(grad, tokens_in.at[me_z], 0)
    own_gates = local_copy(gates, gates_in.at[me_z], 1)
    own_routes = local_copy(routes, routes_in, 2)
    own_pre = local_copy(gate_pre, gate_in, 3)
    own_up = local_copy(up_pre, up_in, 4)

    def weight_copy(i):
        e, b = i // per, lax.rem(i, per)
        where = pl.ds(b * block, block)
        return pltpu.make_async_copy(weights.at[e, where], held.at[e, where], load_sem.at[i])

    own_routes.wait()
    first, second = routes_in[0:1, :], routes_in[1:2, :]
    row8 = lax.broadcasted_iota(jnp.int32, (8, 1), 0)
    lane8 = lax.broadcasted_iota(jnp.int32, (1, span), 1)
    expert_of = me_z * local + row8 // PAD
    slot_of = lax.rem(row8, PAD)
    by_choice = [(route == expert_of) for route in (first, second)]
    named = jnp.where(by_choice[0] | by_choice[1], 1, 0)
    before = jnp.zeros((8, span), jnp.int32)
    for t in range(span - 1):
        before = before + jnp.where(lane8 > t, named[:, t : t + 1], 0)
    fills = (before == slot_of) & (named > 0)
    select = jnp.where(fills, 1.0, 0.0)
    select_by = [jnp.where(fills & choice, 1.0, 0.0) for choice in by_choice]

    own_rows.wait()
    own_gates.wait()
    own_pre.wait()
    own_up.wait()
    for i in range(steps):
        weight_copy(i).start()

    pl.semaphore_wait(barrier, len(peers))
    stage_one = []
    for dz in range(1, groups):
        peer = (me_dp, lax.rem(me_z + dz, groups))
        for ref, s_sem, r_sem in ((tokens_in, send_z, recv_z), (gates_in, send_g, recv_g)):
            copy = pltpu.make_async_remote_copy(
                src_ref=ref.at[me_z], dst_ref=ref.at[me_z],
                send_sem=s_sem.at[dz], recv_sem=r_sem.at[dz],
                device_id=peer, device_id_type=MESH,
            )
            copy.start()
            stage_one.append(copy)

    wide_row = lax.broadcasted_iota(jnp.int32, (full, 1), 0)
    pair_row = lax.broadcasted_iota(jnp.int32, (1, rows), 1)
    spot = (wide_row // 8) * SLOTS + lax.rem(wide_row, PAD)
    real = lax.rem(wide_row, PAD) < SLOTS
    spread = []
    for e in range(local):
        mine = real & (lax.rem(wide_row, 8) // PAD == e)
        spread.append(jnp.where(mine & (spot == pair_row), 1.0, 0.0))
    flip_row = lax.broadcasted_iota(jnp.int32, (rows, 1), 0)
    flip_col = lax.broadcasted_iota(jnp.int32, (1, full), 1)
    flip_spot = (flip_col // 8) * SLOTS + lax.rem(flip_col, PAD)
    flip_real = lax.rem(flip_col, PAD) < SLOTS
    unspread = []
    for e in range(local):
        mine = flip_real & (lax.rem(flip_col, 8) // PAD == e)
        unspread.append(jnp.where(mine & (flip_spot == flip_row), 1.0, 0.0).astype(BF16))

    owner = lax.rem(wide_row, 8) // PAD
    for c in range(0, hidden, 512):
        cols = slice(c, c + 512)
        gate_act = jnp.zeros((full, 512), F32)
        up_act = jnp.zeros((full, 512), F32)
        for e in range(local):
            pick = spread[e].astype(BF16)
            gate_act += jnp.dot(pick, gate_in[e, :, cols], preferred_element_type=F32)
            up_act += jnp.dot(pick, up_in[e, :, cols], preferred_element_type=F32)
        sigmoid_val = jax.nn.sigmoid(gate_act)
        silu_val = gate_act * sigmoid_val
        act = silu_val * up_act
        silu_kept[:, cols] = silu_val
        slope_kept[:, cols] = up_act * sigmoid_val * (1.0 + gate_act * (1.0 - sigmoid_val))
        turned_kept[cols, :] = act.T
        for e in range(local):
            part = jnp.where(owner == e, act, 0.0)
            top = part.astype(BF16)
            rest = (part - top.astype(F32)).astype(BF16)
            for b in range(512 // block):
                at = slice(b * block, (b + 1) * block)
                high[e * per + c // block + b, :full] = top[:, at]
                high[e * per + c // block + b, full:] = rest[:, at]

    def forward_step(i, flip):
        e, b = i // per, lax.rem(i, per)
        weight_copy(i).wait()
        left = high[i]
        for n in range(0, width, 512):
            right = held[e, pl.ds(pl.multiple_of(b * block, block), block), n : n + 512]
            totals[:, n : n + 512] += jnp.dot(left, right, preferred_element_type=F32)
            if flip:
                flips[i, n : n + 512, :] = right.T

    def forward_steps(low, top):
        def body(flip, i, carry):
            forward_step(i, flip)
            return carry

        middle = min(max(low, flipped), top)
        if middle > low:
            lax.fori_loop(low, middle, functools.partial(body, True), 0)
        if top > middle:
            lax.fori_loop(middle, top, functools.partial(body, False), 0)

    totals[...] = jnp.zeros_like(totals)
    forward_steps(0, early[0])

    for copy in stage_one:
        copy.wait_recv()
    slots = jnp.zeros((8, width), F32)
    gate = jnp.zeros((8, 1), F32)
    for z in range(groups):
        got = tokens_in[z].astype(F32)
        got_gate = gates_in[z].astype(F32)
        for t in range(tokens):
            at = z * tokens + t
            slots = slots + select[:, at : at + 1] * got[t : t + 1, :]
            for k in range(2):
                gate = gate + select_by[k][:, at : at + 1] * got_gate[t : t + 1, k : k + 1]
    gate_wide = jnp.broadcast_to(gate, (8, LANES))
    base = pl.multiple_of(me_dp * 16, 16)
    table[pl.ds(base, 16), :half] = jnp.concatenate(
        [slots[:, :half], slots[:, half:]], axis=0
    ).astype(BF16)
    table[pl.ds(base, 16), half:] = jnp.concatenate([gate_wide, gate_wide], axis=0).astype(BF16)

    def block_copy(dp_index, target, piece, s_sem, r_sem):
        where = table.at[pl.ds(dp_index * 16, 16), pl.ds(pieces[piece], pieces[piece + 1] - pieces[piece])]
        copy = pltpu.make_async_remote_copy(
            src_ref=where, dst_ref=where, send_sem=s_sem, recv_sem=r_sem,
            device_id=(target, me_z), device_id_type=MESH,
        )
        copy.start()
        return copy

    count = len(pieces) - 1
    stage_two = {}
    stage_three = {}
    for p in range(count):
        for dc in range(1, chips):
            target = lax.rem(chip + dc, chips) * CORES + core
            stage_two[p, dc] = block_copy(me_dp, target, p, send_c.at[p, dc], recv_c.at[p, dc])
        stage_three[p, 0] = block_copy(me_dp, partner, p, send_p.at[p, 0], recv_p.at[p, 0])

    forward_steps(early[0], early[1])

    for p in range(count):
        for dc in range(1, chips):
            stage_two[p, dc].wait_recv()
            source = lax.rem(chip - dc + chips, chips) * CORES + core
            stage_three[p, dc] = block_copy(source, partner, p, send_p.at[p, dc], recv_p.at[p, dc])

    forward_steps(early[1], steps)

    for copy in stage_three.values():
        copy.wait_recv()

    part = jnp.zeros((full, LANES), F32)
    for h in range(2):
        for n in range(0, half, 512):
            got = table[:, n : n + 512].astype(F32).reshape(n_dp, 16, 512)
            got = got[:, h * 8 : h * 8 + 8].reshape(full, 512)
            at = slice(h * half + n, h * half + n + 512)
            picked[:, at] = got.astype(BF16)
            term = got * (totals[:full, at] + totals[full:, at])
            for q in range(0, 512, LANES):
                part = part + term[:, q : q + LANES]
    rows_out[...] = picked[...]
    part = jnp.sum(part, axis=1, keepdims=True)
    lane = lax.broadcasted_iota(jnp.int32, (full, LANES), 1)
    sums = jnp.sum(jnp.where(lane == wide_row, part, 0.0), axis=0, keepdims=True)
    sums_own[...] = sums
    sums_all[me] = sums
    last = []
    for off in range(1, total):
        other = lax.rem(me + off, total)
        copy = pltpu.make_async_remote_copy(
            src_ref=sums_own, dst_ref=sums_all.at[me],
            send_sem=send_s.at[off], recv_sem=recv_s.at[off],
            device_id=(other // groups, lax.rem(other, groups)), device_id_type=MESH,
        )
        copy.start()
        last.append(copy)

    scale = table[:, half:].astype(F32).reshape(n_dp, 16, LANES)[:, :8].reshape(full, LANES)
    scale_row = scale.T[0:1, :]
    scale_col = scale[:, 0:1]
    col = lax.broadcasted_iota(jnp.int32, (1, full), 1)
    for e in range(local):
        factor = jnp.where(lax.rem(col, 8) // PAD == e, scale_row, 0.0)
        turned_out[e] = (turned_kept[...] * factor).astype(BF16)
    for c in range(0, hidden, 512):
        cols = slice(c, c + 512)
        both = []
        for e in range(local):
            i = e * per + c // block
            if i < flipped:
                both.append(jnp.dot(picked[...], flips[i], preferred_element_type=F32))
            else:
                both.append(
                    lax.dot_general(
                        picked[...], held[e, cols], (((1,), (1,)), ((), ())),
                        preferred_element_type=F32,
                    )
                )
        proj = both[0]
        for e in range(1, local):
            proj = jnp.where(owner == e, both[e], proj)
        grad_hidden = scale_col * proj
        gate_grad = (grad_hidden * slope_kept[:, cols]).astype(BF16)
        up_grad = (grad_hidden * silu_kept[:, cols]).astype(BF16)
        for e in range(local):
            for ref, value in ((grad_gate_out, gate_grad), (grad_up_out, up_grad)):
                ref[e, :, cols] = jnp.dot(
                    unspread[e], value, preferred_element_type=F32
                ).astype(BF16)

    for copy in last:
        copy.wait_recv()
    sums_by = []
    for z in range(groups):
        acc = sums_all[z]
        for d in range(1, n_dp):
            acc = acc + sums_all[d * groups + z]
        sums_by.append(acc)
    out_row = lax.broadcasted_iota(jnp.int32, sums_out.shape, 0)
    out_col = lax.broadcasted_iota(jnp.int32, sums_out.shape, 1)
    spots = lax.broadcasted_iota(jnp.int32, (1, LANES), 1)
    result = jnp.zeros(sums_out.shape, F32)
    for k, route in enumerate((first, second)):
        ahead = jnp.zeros((1, span), jnp.int32)
        for t in range(span - 1):
            same = (first[:, t : t + 1] == route) | (second[:, t : t + 1] == route)
            ahead = ahead + jnp.where((lane8 > t) & same, 1, 0)
        for t in range(tokens):
            here = lane8 == me_z * tokens + t
            expert = jnp.sum(jnp.where(here, route, 0), axis=1, keepdims=True)
            place = jnp.sum(jnp.where(here, ahead, 0), axis=1, keepdims=True)
            value = jnp.zeros((1, LANES), F32)
            for z in range(groups):
                offset = expert - z * local
                code = jnp.where(
                    (offset >= 0) & (offset < local), me_dp * 8 + offset * PAD + place, -1
                )
                value = value + jnp.where(spots == code, sums_by[z], 0.0)
            value = jnp.sum(value, axis=1, keepdims=True)
            result = jnp.where((out_row == t) & (out_col == k), value, result)
    sums_out[...] = result
    for copy in stage_one + list(stage_two.values()) + list(stage_three.values()) + last:
        copy.wait_send()


def finish(
    block, rows_in, turned, gate_grad, up_grad, sums,
    grad_sums, grad_gate, grad_up, grad_down, made, small_sem, out_sem,
):
    local, hidden, _ = turned.shape
    width = rows_in.shape[1]
    per = hidden // block
    small = []
    for at, (src, dst) in enumerate(
        ((sums, grad_sums), (gate_grad, grad_gate), (up_grad, grad_up))
    ):
        copy = pltpu.make_async_copy(src, dst, small_sem.at[at])
        copy.start()
        small.append(copy)

    def out_copy(i):
        e, b = i // per, lax.rem(i, per)
        where = pl.ds(b * block, block)
        return pltpu.make_async_copy(made.at[e, where], grad_down.at[e, where], out_sem.at[i])

    def body(i, carry):
        e, b = i // per, lax.rem(i, per)
        where = pl.ds(pl.multiple_of(b * block, block), block)
        left = turned[e, where, :]
        for n in range(0, width, 512):
            made[e, where, n : n + 512] = jnp.dot(
                left, rows_in[:, n : n + 512], preferred_element_type=F32
            ).astype(BF16)
        out_copy(i).start()
        return carry

    lax.fori_loop(0, local * per, body, 0, unroll=2)

    def drain(i, carry):
        out_copy(i).wait()
        return carry

    lax.fori_loop(0, local * per, drain, 0)
    for copy in small:
        copy.wait()


def fused_device(out_grad, routes, gate_values, gate_pre, up_pre, w_down):
    n_dp, groups = lax.axis_size("dp"), lax.axis_size("expert")
    tokens, width = out_grad.shape
    local, rows, hidden = gate_pre.shape
    block = 512
    total = n_dp * groups
    full = n_dp * 8
    half = width // 2
    chips = n_dp // CORES
    pieces = (0, half + LANES)
    count = len(pieces) - 1
    steps = local * hidden // block
    early = (steps // 3, steps - 1)
    flipped = steps
    span = groups * tokens

    vmem = pl.BlockSpec(memory_space=pltpu.VMEM)
    hbm = pl.BlockSpec(memory_space=pltpu.HBM)
    dma = pltpu.SemaphoreType.DMA
    scratch = pltpu.VMEM
    placed = [
        pltpu.with_memory_space_constraint(ref, pltpu.HBM)
        for ref in (out_grad, routes.T, gate_values, gate_pre, up_pre, w_down)
    ]
    rows_in, turned, gate_grad, up_grad, sums = pl.pallas_call(
        functools.partial(gather_project, n_dp, groups, local, rows, block, pieces, early, flipped),
        out_shape=(
            pltpu.VMEM((full, width), BF16),
            pltpu.VMEM((local, hidden, full), BF16),
            pltpu.VMEM(gate_pre.shape, BF16),
            pltpu.VMEM(up_pre.shape, BF16),
            pltpu.VMEM((tokens, 2), F32),
        ),
        in_specs=[hbm] * 6,
        out_specs=(vmem,) * 5,
        scratch_shapes=[
            scratch((local, hidden, width), BF16),
            scratch((groups, tokens, width), BF16),
            scratch((groups, tokens, 2), BF16),
            scratch((2, span), jnp.int32),
            scratch(gate_pre.shape, BF16),
            scratch(up_pre.shape, BF16),
            scratch((n_dp * 16, half + LANES), BF16),
            scratch((full, width), BF16),
            scratch((steps, 2 * full, block), BF16),
            scratch((2 * full, width), F32),
            scratch((flipped, width, block), BF16),
            scratch((full, hidden), F32),
            scratch((full, hidden), F32),
            scratch((hidden, full), F32),
            scratch((1, LANES), F32),
            scratch((total, 1, LANES), F32),
            dma((steps,)),
            dma((5,)),
            dma((groups,)),
            dma((groups,)),
            dma((groups,)),
            dma((groups,)),
            dma((count, chips)),
            dma((count, chips)),
            dma((count, chips)),
            dma((count, chips)),
            dma((total,)),
            dma((total,)),
        ],
        compiler_params=pltpu.CompilerParams(
            collective_id=0, has_side_effects=True, vmem_limit_bytes=59 << 20
        ),
        name="gather_project",
    )(*placed)

    piece = 256
    return pl.pallas_call(
        functools.partial(finish, piece),
        out_shape=(
            jax.ShapeDtypeStruct((tokens, 2), F32),
            jax.ShapeDtypeStruct(gate_pre.shape, BF16),
            jax.ShapeDtypeStruct(up_pre.shape, BF16),
            jax.ShapeDtypeStruct(w_down.shape, BF16),
        ),
        in_specs=[vmem] * 5,
        out_specs=(hbm,) * 4,
        scratch_shapes=[
            scratch((local, hidden, width), BF16),
            dma((3,)),
            dma((local * hidden // piece,)),
        ],
        compiler_params=pltpu.CompilerParams(vmem_limit_bytes=52 << 20),
        name="finish",
    )(rows_in, turned, gate_grad, up_grad, sums)


def per_device(out_grad, routes, gate_values, gate_pre, up_pre, w_down):
    fits = fused_fits(
        lax.axis_size("dp"), lax.axis_size("expert"), *out_grad.shape, *gate_pre.shape
    )
    chosen = fused_device if fits else general_device
    return chosen(out_grad, routes, gate_values, gate_pre, up_pre, w_down)


def solution(mesh):
    return jax.shard_map(
        per_device,
        mesh=mesh,
        in_specs=(
            P(("dp", "expert"), None),
            P("dp", None),
            P(("dp", "expert"), None),
            P("expert", None, "dp"),
            P("expert", None, "dp"),
            P("expert", "dp", None),
        ),
        out_specs=(
            P(("dp", "expert"), None),
            P("expert", None, "dp"),
            P("expert", None, "dp"),
            P("expert", "dp", None),
        ),
        check_vma=False,
    )
```

```python
import functools

import jax
import jax.numpy as jnp
from jax import lax
from jax.experimental import pallas as pl
from jax.experimental.pallas import tpu as pltpu
from jax.sharding import PartitionSpec as P

SLOTS = 3


def expert_terms(gate_piece, up_piece, weights, rows_in, gate_row):
    projected = jnp.einsum("erd,efd->erf", rows_in, weights, preferred_element_type=jnp.float32)
    gate_act = gate_piece.astype(jnp.float32)
    up_act = up_piece.astype(jnp.float32)
    sigmoid_val = jax.nn.sigmoid(gate_act)
    silu_val = gate_act * sigmoid_val
    hidden = silu_val * up_act
    partial_value = jnp.sum(hidden * projected, axis=2)
    scale_col = gate_row.astype(jnp.float32)[:, :, None]
    weighted = (scale_col * hidden).astype(jnp.bfloat16)
    down_term = jnp.einsum("erf,erd->efd", weighted, rows_in, preferred_element_type=jnp.float32)
    grad_hidden = scale_col * projected
    grad_gate = (
        grad_hidden * up_act * sigmoid_val * (1.0 + gate_act * (1.0 - sigmoid_val))
    ).astype(jnp.bfloat16)
    grad_up = (grad_hidden * silu_val).astype(jnp.bfloat16)
    return (partial_value, grad_gate, grad_up, down_term)


def general_device(out_grad, routes, gate_values, gate_pre, up_pre, w_down):
    groups = lax.axis_size("expert")
    local_count = gate_pre.shape[0]
    experts = local_count * groups
    tok_count = out_grad.shape[0]
    my_rank = lax.axis_index("expert")
    flat_routes = routes.reshape(-1)
    onehot = (flat_routes[:, None] == jnp.arange(experts, dtype=jnp.int32)[None, :]).astype(
        jnp.int32
    )
    position = jnp.sum((jnp.cumsum(onehot, axis=0) - 1) * onehot, axis=1)
    own_expert = lax.dynamic_slice_in_dim(flat_routes, my_rank * tok_count * 2, tok_count * 2)
    own_position = lax.dynamic_slice_in_dim(position, my_rank * tok_count * 2, tok_count * 2)
    target = own_expert * SLOTS + own_position
    selector = target[:, None] == jnp.arange(experts * SLOTS, dtype=jnp.int32)[None, :]
    picker = selector.astype(jnp.bfloat16).T
    pair_rows = jnp.repeat(out_grad, 2, axis=0)
    send_rows = (
        jnp.dot(picker, pair_rows, preferred_element_type=jnp.float32)
        .astype(jnp.bfloat16)
        .reshape(experts, SLOTS, -1)
    )
    send_gates = (
        jnp.dot(picker, gate_values.reshape(-1, 1), preferred_element_type=jnp.float32)
        .astype(jnp.bfloat16)
        .reshape(experts, SLOTS)
    )
    got_rows, got_gates = (
        lax.all_to_all(send_rows, "expert", split_axis=0, concat_axis=0, tiled=True),
        lax.all_to_all(send_gates, "expert", split_axis=0, concat_axis=0, tiled=True),
    )
    dispatched = jnp.sum(
        got_rows.reshape(groups, local_count, SLOTS, -1).astype(jnp.float32), axis=0
    ).astype(jnp.bfloat16)
    slot_gate = jnp.sum(
        got_gates.reshape(groups, local_count, SLOTS).astype(jnp.float32), axis=0
    ).astype(jnp.bfloat16)
    all_rows, all_gates = (
        lax.all_gather(dispatched, "dp", axis=1, tiled=True),
        lax.all_gather(slot_gate, "dp", axis=1, tiled=True),
    )
    partial_value, grad_gate_pre, grad_up_pre, down_sum = expert_terms(
        gate_pre, up_pre, w_down, all_rows, all_gates
    )
    grad_down = down_sum.astype(jnp.bfloat16)
    own_sums = lax.psum_scatter(partial_value, "dp", scatter_dimension=1, tiled=True)
    score_table = lax.all_gather(own_sums, "expert", axis=0, tiled=True)
    picked = jnp.sum(jnp.where(selector, score_table.reshape(1, -1), 0.0), axis=1)
    grad_gates = picked.reshape(tok_count, 2)
    return (grad_gates, grad_gate_pre, grad_up_pre, grad_down)


LANES = 128
CORES = 2
PAD = 4
MESH = pl.DeviceIdType.MESH
BF16 = jnp.bfloat16
F32 = jnp.float32


def pow2(n):
    return n & (n - 1) == 0


def far_first(n):
    return sorted(range(1, n), reverse=True)


def fused_fits(n_dp, groups, tokens, width, local, rows, hidden):
    return (
        n_dp % CORES == 0
        and n_dp > CORES
        and groups > 1
        and pow2(groups)
        and pow2(n_dp)
        and local * PAD == 8
        and rows == n_dp * SLOTS
        and n_dp * 8 <= LANES
        and groups * tokens <= LANES
        and width % (4 * LANES) == 0
        and hidden % 512 == 0
        and n_dp * groups <= 64
        and local * hidden * width * 2 <= 26 << 20
    )


def gather_project(
    n_dp, groups, local, rows, block, pieces, early, flipped,
    grad, routes, gates, gate_pre, up_pre, weights,
    rows_out, turned_out, grad_gate_out, grad_up_out, sums_out,
    held, tokens_in, gates_in, routes_in, gate_in, up_in,
    table, high, totals, flips, silu_kept, slope_kept, turned_kept,
    sums_own, sums_all,
    load_sem, in_sem, send_z, recv_z, send_g, recv_g, send_c, recv_c, send_p, recv_p,
    send_s, recv_s,
):
    me_dp, me_z = lax.axis_index("dp"), lax.axis_index("expert")
    total = n_dp * groups
    me = me_dp * groups + me_z
    chips = n_dp // CORES
    chip, core = me_dp // CORES, lax.rem(me_dp, CORES)
    partner = chip * CORES + (1 - core)
    tokens, width = grad.shape
    hidden = held.shape[1]
    per = hidden // block
    steps = local * per
    half = width // 2
    full = n_dp * 8
    span = tokens * groups

    barrier = pltpu.get_barrier_semaphore()
    peers = [(me_dp, me_z ^ dz) for dz in far_first(groups)]
    peers += [((chip ^ dc) * CORES + core, me_z) for dc in far_first(chips)]
    peers += [(partner, me_z)]
    for peer in peers:
        pl.semaphore_signal(barrier, inc=1, device_id=peer, device_id_type=MESH)

    def local_copy(src, dst, at):
        copy = pltpu.make_async_copy(src, dst, in_sem.at[at])
        copy.start()
        return copy

    own_rows = local_copy(grad, tokens_in.at[me_z], 0)
    own_gates = local_copy(gates, gates_in.at[me_z], 1)
    own_routes = local_copy(routes, routes_in, 2)
    own_pre = local_copy(gate_pre, gate_in, 3)
    own_up = local_copy(up_pre, up_in, 4)

    def weight_copy(i):
        e, b = i // per, lax.rem(i, per)
        where = pl.ds(b * block, block)
        return pltpu.make_async_copy(weights.at[e, where], held.at[e, where], load_sem.at[i])

    own_routes.wait()
    first, second = routes_in[0:1, :], routes_in[1:2, :]
    row8 = lax.broadcasted_iota(jnp.int32, (8, 1), 0)
    lane8 = lax.broadcasted_iota(jnp.int32, (1, span), 1)
    expert_of = me_z * local + row8 // PAD
    slot_of = lax.rem(row8, PAD)
    by_choice = [(route == expert_of) for route in (first, second)]
    named = jnp.where(by_choice[0] | by_choice[1], 1, 0)
    before = jnp.zeros((8, span), jnp.int32)
    for t in range(span - 1):
        before = before + jnp.where(lane8 > t, named[:, t : t + 1], 0)
    fills = (before == slot_of) & (named > 0)
    select = jnp.where(fills, 1.0, 0.0)
    select_by = [jnp.where(fills & choice, 1.0, 0.0) for choice in by_choice]

    own_rows.wait()
    own_gates.wait()
    weight_copy(0).start()
    own_pre.wait()
    own_up.wait()
    for i in range(1, steps):
        weight_copy(i).start()

    pl.semaphore_wait(barrier, len(peers))
    stage_one = []
    for dz in far_first(groups):
        peer = (me_dp, me_z ^ dz)
        for ref, s_sem, r_sem in ((tokens_in, send_z, recv_z), (gates_in, send_g, recv_g)):
            copy = pltpu.make_async_remote_copy(
                src_ref=ref.at[me_z], dst_ref=ref.at[me_z],
                send_sem=s_sem.at[dz], recv_sem=r_sem.at[dz],
                device_id=peer, device_id_type=MESH,
            )
            copy.start()
            stage_one.append(copy)

    wide_row = lax.broadcasted_iota(jnp.int32, (full, 1), 0)
    pair_row = lax.broadcasted_iota(jnp.int32, (1, rows), 1)
    spot = (wide_row // 8) * SLOTS + lax.rem(wide_row, PAD)
    real = lax.rem(wide_row, PAD) < SLOTS
    spread = []
    for e in range(local):
        mine = real & (lax.rem(wide_row, 8) // PAD == e)
        spread.append(jnp.where(mine & (spot == pair_row), 1.0, 0.0))
    flip_row = lax.broadcasted_iota(jnp.int32, (rows, 1), 0)
    flip_col = lax.broadcasted_iota(jnp.int32, (1, full), 1)
    flip_spot = (flip_col // 8) * SLOTS + lax.rem(flip_col, PAD)
    flip_real = lax.rem(flip_col, PAD) < SLOTS
    unspread = []
    for e in range(local):
        mine = flip_real & (lax.rem(flip_col, 8) // PAD == e)
        unspread.append(jnp.where(mine & (flip_spot == flip_row), 1.0, 0.0).astype(BF16))

    owner = lax.rem(wide_row, 8) // PAD
    for c in range(0, hidden, 512):
        cols = slice(c, c + 512)
        gate_act = jnp.zeros((full, 512), F32)
        up_act = jnp.zeros((full, 512), F32)
        for e in range(local):
            pick = spread[e].astype(BF16)
            gate_act += jnp.dot(pick, gate_in[e, :, cols], preferred_element_type=F32)
            up_act += jnp.dot(pick, up_in[e, :, cols], preferred_element_type=F32)
        sigmoid_val = jax.nn.sigmoid(gate_act)
        silu_val = gate_act * sigmoid_val
        act = silu_val * up_act
        silu_kept[:, cols] = silu_val
        slope_kept[:, cols] = up_act * sigmoid_val * (1.0 + gate_act * (1.0 - sigmoid_val))
        turned_kept[cols, :] = act.T
        for e in range(local):
            part = jnp.where(owner == e, act, 0.0)
            top = part.astype(BF16)
            rest = (part - top.astype(F32)).astype(BF16)
            for b in range(512 // block):
                at = slice(b * block, (b + 1) * block)
                high[e * per + c // block + b, :full] = top[:, at]
                high[e * per + c // block + b, full:] = rest[:, at]

    eye_row = lax.broadcasted_iota(jnp.int32, (256, 256), 0)
    eye_col = lax.broadcasted_iota(jnp.int32, (256, 256), 1)
    eye = jnp.where(eye_row == eye_col, 1.0, 0.0).astype(BF16)
    by_product = (width // 1024,)

    def forward_step(i, flip):
        e, b = i // per, lax.rem(i, per)
        weight_copy(i).wait()
        left = high[i]
        for n in range(0, width, 512):
            right = held[e, pl.ds(pl.multiple_of(b * block, block), block), n : n + 512]
            totals[:, n : n + 512] += jnp.dot(left, right, preferred_element_type=F32)
            if flip and n // 512 in by_product:
                for q in range(0, 512, 256):
                    flips[i, n + q : n + q + 256, :] = lax.dot_general(
                        eye, right[:, q : q + 256], (((1,), (1,)), ((), ())),
                        preferred_element_type=F32,
                    ).astype(BF16)
            elif flip:
                flips[i, n : n + 512, :] = right.T

    def forward_steps(low, top):
        def body(flip, i, carry):
            forward_step(i, flip)
            return carry

        middle = min(max(low, flipped), top)
        if middle > low:
            lax.fori_loop(low, middle, functools.partial(body, True), 0)
        if top > middle:
            lax.fori_loop(middle, top, functools.partial(body, False), 0)

    totals[...] = jnp.zeros_like(totals)
    forward_steps(0, early[0])

    for copy in stage_one:
        copy.wait_recv()
    slots = jnp.zeros((8, width), F32)
    gate = jnp.zeros((8, 1), F32)
    for z in range(groups):
        got = tokens_in[z].astype(F32)
        got_gate = gates_in[z].astype(F32)
        for t in range(tokens):
            at = z * tokens + t
            slots = slots + select[:, at : at + 1] * got[t : t + 1, :]
            for k in range(2):
                gate = gate + select_by[k][:, at : at + 1] * got_gate[t : t + 1, k : k + 1]
    gate_wide = jnp.broadcast_to(gate, (8, LANES))
    base = pl.multiple_of(me_dp * 16, 16)
    table[pl.ds(base, 16), :half] = jnp.concatenate(
        [slots[:, :half], slots[:, half:]], axis=0
    ).astype(BF16)
    table[pl.ds(base, 16), half:] = jnp.concatenate([gate_wide, gate_wide], axis=0).astype(BF16)

    def block_copy(dp_index, target, piece, s_sem, r_sem):
        where = table.at[pl.ds(dp_index * 16, 16), pl.ds(pieces[piece], pieces[piece + 1] - pieces[piece])]
        copy = pltpu.make_async_remote_copy(
            src_ref=where, dst_ref=where, send_sem=s_sem, recv_sem=r_sem,
            device_id=(target, me_z), device_id_type=MESH,
        )
        copy.start()
        return copy

    count = len(pieces) - 1
    stage_two = {}
    stage_three = {}
    for p in range(count):
        for dc in far_first(chips):
            target = (chip ^ dc) * CORES + core
            stage_two[p, dc] = block_copy(me_dp, target, p, send_c.at[p, dc], recv_c.at[p, dc])
        stage_three[p, 0] = block_copy(me_dp, partner, p, send_p.at[p, 0], recv_p.at[p, 0])

    forward_steps(early[0], early[1])

    for p in range(count):
        for dc in range(1, chips):
            stage_two[p, dc].wait_recv()
            source = (chip ^ dc) * CORES + core
            stage_three[p, dc] = block_copy(source, partner, p, send_p.at[p, dc], recv_p.at[p, dc])

    forward_steps(early[1], steps)

    for n in range(0, width, 512):
        totals[:full, n : n + 512] += totals[full:, n : n + 512]

    for copy in stage_three.values():
        copy.wait_recv()

    part = jnp.zeros((full, LANES), F32)
    for h in range(2):
        for n in range(0, half, 512):
            got = table[:, n : n + 512].astype(F32).reshape(n_dp, 16, 512)
            got = got[:, h * 8 : h * 8 + 8].reshape(full, 512)
            at = slice(h * half + n, h * half + n + 512)
            rows_out[:, at] = got.astype(BF16)
            term = got * totals[:full, at]
            for q in range(0, 512, LANES):
                part = part + term[:, q : q + LANES]
    part = jnp.sum(part, axis=1, keepdims=True)
    lane = lax.broadcasted_iota(jnp.int32, (full, LANES), 1)
    sums = jnp.sum(jnp.where(lane == wide_row, part, 0.0), axis=0, keepdims=True)
    sums_own[...] = sums
    sums_all[me] = sums
    last = []
    offsets = [(dp, z) for z in range(groups) for dp in range(n_dp)][1:]
    for off, (dp, z) in sorted(enumerate(offsets, 1), reverse=True):
        copy = pltpu.make_async_remote_copy(
            src_ref=sums_own, dst_ref=sums_all.at[me],
            send_sem=send_s.at[off], recv_sem=recv_s.at[off],
            device_id=(me_dp ^ dp, me_z ^ z), device_id_type=MESH,
        )
        copy.start()
        last.append(copy)

    scale = table[:, half:].astype(F32).reshape(n_dp, 16, LANES)[:, :8].reshape(full, LANES)
    scale_row = scale.T[0:1, :]
    scale_col = scale[:, 0:1]
    col = lax.broadcasted_iota(jnp.int32, (1, full), 1)
    for e in range(local):
        factor = jnp.where(lax.rem(col, 8) // PAD == e, scale_row, 0.0)
        turned_out[e] = (turned_kept[...] * factor).astype(BF16)
    for c in range(0, hidden, 512):
        cols = slice(c, c + 512)
        both = []
        for e in range(local):
            i = e * per + c // block
            if i < flipped:
                both.append(jnp.dot(rows_out[...], flips[i], preferred_element_type=F32))
            else:
                both.append(
                    lax.dot_general(
                        rows_out[...], held[e, cols], (((1,), (1,)), ((), ())),
                        preferred_element_type=F32,
                    )
                )
        proj = both[0]
        for e in range(1, local):
            proj = jnp.where(owner == e, both[e], proj)
        grad_hidden = scale_col * proj
        gate_grad = (grad_hidden * slope_kept[:, cols]).astype(BF16)
        up_grad = (grad_hidden * silu_kept[:, cols]).astype(BF16)
        for e in range(local):
            for ref, value in ((grad_gate_out, gate_grad), (grad_up_out, up_grad)):
                ref[e, :, cols] = jnp.dot(
                    unspread[e], value, preferred_element_type=F32
                ).astype(BF16)

    out_row = lax.broadcasted_iota(jnp.int32, sums_out.shape, 0)
    out_col = lax.broadcasted_iota(jnp.int32, sums_out.shape, 1)
    spots = lax.broadcasted_iota(jnp.int32, (1, LANES), 1)
    masks = {}
    for k, route in enumerate((first, second)):
        ahead = jnp.zeros((1, span), jnp.int32)
        for t in range(span - 1):
            same = (first[:, t : t + 1] == route) | (second[:, t : t + 1] == route)
            ahead = ahead + jnp.where((lane8 > t) & same, 1, 0)
        for t in range(tokens):
            here = lane8 == me_z * tokens + t
            expert = jnp.sum(jnp.where(here, route, 0), axis=1, keepdims=True)
            place = jnp.sum(jnp.where(here, ahead, 0), axis=1, keepdims=True)
            for z in range(groups):
                offset = expert - z * local
                code = jnp.where(
                    (offset >= 0) & (offset < local), me_dp * 8 + offset * PAD + place, -1
                )
                masks[t, k, z] = jnp.where(spots == code, 1.0, 0.0)
    for copy in last:
        copy.wait_recv()
    sums_by = []
    for z in range(groups):
        acc = sums_all[z]
        for d in range(1, n_dp):
            acc = acc + sums_all[d * groups + z]
        sums_by.append(acc)
    result = jnp.zeros(sums_out.shape, F32)
    for t in range(tokens):
        for k in range(2):
            value = jnp.zeros((1, LANES), F32)
            for z in range(groups):
                value = value + jnp.where(masks[t, k, z] > 0.5, sums_by[z], 0.0)
            value = jnp.sum(value, axis=1, keepdims=True)
            result = jnp.where((out_row == t) & (out_col == k), value, result)
    sums_out[...] = result
    for copy in stage_one + list(stage_two.values()) + list(stage_three.values()) + last:
        copy.wait_send()


def finish(
    block, rows_in, turned, gate_grad, up_grad, sums,
    grad_sums, grad_gate, grad_up, grad_down, made, small_sem, out_sem,
):
    local, hidden, _ = turned.shape
    width = rows_in.shape[1]
    per = hidden // block
    small = []
    for at, (src, dst) in enumerate(
        ((sums, grad_sums), (gate_grad, grad_gate), (up_grad, grad_up))
    ):
        copy = pltpu.make_async_copy(src, dst, small_sem.at[at])
        copy.start()
        small.append(copy)

    def out_copy(i):
        e, b = i // per, lax.rem(i, per)
        where = pl.ds(b * block, block)
        return pltpu.make_async_copy(made.at[e, where], grad_down.at[e, where], out_sem.at[i])

    def make(e, where):
        left = turned[e, where, :]
        for n in range(0, width, 512):
            made[e, where, n : n + 512] = jnp.dot(
                left, rows_in[:, n : n + 512], preferred_element_type=F32
            ).astype(BF16)

    def body(i, carry):
        e, b = i // per, lax.rem(i, per)
        make(e, pl.ds(pl.multiple_of(b * block, block), block))
        out_copy(i).start()
        return carry

    part = block // 2
    first = []
    for q in range(2):
        where = pl.ds(q * part, part)
        make(0, where)
        copy = pltpu.make_async_copy(
            made.at[0, where], grad_down.at[0, where], small_sem.at[3 + q]
        )
        copy.start()
        first.append(copy)
    body(1, 0)
    lax.fori_loop(2, local * per, body, 0, unroll=2)

    def drain(i, carry):
        out_copy(i).wait()
        return carry

    lax.fori_loop(1, local * per, drain, 0)
    for copy in small + first:
        copy.wait()


def fused_device(out_grad, routes, gate_values, gate_pre, up_pre, w_down):
    n_dp, groups = lax.axis_size("dp"), lax.axis_size("expert")
    tokens, width = out_grad.shape
    local, rows, hidden = gate_pre.shape
    block = 512
    total = n_dp * groups
    full = n_dp * 8
    half = width // 2
    chips = n_dp // CORES
    pieces = (0, half + LANES)
    count = len(pieces) - 1
    steps = local * hidden // block
    early = (steps // 3, steps - 1)
    flipped = steps
    span = groups * tokens

    vmem = pl.BlockSpec(memory_space=pltpu.VMEM)
    hbm = pl.BlockSpec(memory_space=pltpu.HBM)
    dma = pltpu.SemaphoreType.DMA
    scratch = pltpu.VMEM
    placed = [
        pltpu.with_memory_space_constraint(ref, pltpu.HBM)
        for ref in (out_grad, routes.T, gate_values, gate_pre, up_pre, w_down)
    ]
    rows_in, turned, gate_grad, up_grad, sums = pl.pallas_call(
        functools.partial(gather_project, n_dp, groups, local, rows, block, pieces, early, flipped),
        out_shape=(
            pltpu.VMEM((full, width), BF16),
            pltpu.VMEM((local, hidden, full), BF16),
            pltpu.VMEM(gate_pre.shape, BF16),
            pltpu.VMEM(up_pre.shape, BF16),
            pltpu.VMEM((tokens, 2), F32),
        ),
        in_specs=[hbm] * 6,
        out_specs=(vmem,) * 5,
        scratch_shapes=[
            scratch((local, hidden, width), BF16),
            scratch((groups, tokens, width), BF16),
            scratch((groups, tokens, 2), BF16),
            scratch((2, span), jnp.int32),
            scratch(gate_pre.shape, BF16),
            scratch(up_pre.shape, BF16),
            scratch((n_dp * 16, half + LANES), BF16),
            scratch((steps, 2 * full, block), BF16),
            scratch((2 * full, width), F32),
            scratch((flipped, width, block), BF16),
            scratch((full, hidden), F32),
            scratch((full, hidden), F32),
            scratch((hidden, full), F32),
            scratch((1, LANES), F32),
            scratch((total, 1, LANES), F32),
            dma((steps,)),
            dma((5,)),
            dma((groups,)),
            dma((groups,)),
            dma((groups,)),
            dma((groups,)),
            dma((count, chips)),
            dma((count, chips)),
            dma((count, chips)),
            dma((count, chips)),
            dma((total,)),
            dma((total,)),
        ],
        compiler_params=pltpu.CompilerParams(
            collective_id=0, has_side_effects=True, vmem_limit_bytes=59 << 20
        ),
        name="gather_project",
    )(*placed)

    piece = 256
    return pl.pallas_call(
        functools.partial(finish, piece),
        out_shape=(
            jax.ShapeDtypeStruct((tokens, 2), F32),
            jax.ShapeDtypeStruct(gate_pre.shape, BF16),
            jax.ShapeDtypeStruct(up_pre.shape, BF16),
            jax.ShapeDtypeStruct(w_down.shape, BF16),
        ),
        in_specs=[vmem] * 5,
        out_specs=(hbm,) * 4,
        scratch_shapes=[
            scratch((local, hidden, width), BF16),
            dma((5,)),
            dma((local * hidden // piece,)),
        ],
        compiler_params=pltpu.CompilerParams(vmem_limit_bytes=52 << 20),
        name="finish",
    )(rows_in, turned, gate_grad, up_grad, sums)


def per_device(out_grad, routes, gate_values, gate_pre, up_pre, w_down):
    fits = fused_fits(
        lax.axis_size("dp"), lax.axis_size("expert"), *out_grad.shape, *gate_pre.shape
    )
    chosen = fused_device if fits else general_device
    return chosen(out_grad, routes, gate_values, gate_pre, up_pre, w_down)


def solution(mesh):
    return jax.shard_map(
        per_device,
        mesh=mesh,
        in_specs=(
            P(("dp", "expert"), None),
            P("dp", None),
            P(("dp", "expert"), None),
            P("expert", None, "dp"),
            P("expert", None, "dp"),
            P("expert", "dp", None),
        ),
        out_specs=(
            P(("dp", "expert"), None),
            P("expert", None, "dp"),
            P("expert", None, "dp"),
            P("expert", "dp", None),
        ),
        check_vma=False,
    )
```

```python
import functools

import jax
import jax.numpy as jnp
from jax import lax
from jax.experimental import pallas as pl
from jax.experimental.pallas import tpu as pltpu
from jax.sharding import PartitionSpec as P

SLOTS = 3


def expert_terms(gate_piece, up_piece, weights, rows_in, gate_row):
    projected = jnp.einsum("erd,efd->erf", rows_in, weights, preferred_element_type=jnp.float32)
    gate_act = gate_piece.astype(jnp.float32)
    up_act = up_piece.astype(jnp.float32)
    sigmoid_val = jax.nn.sigmoid(gate_act)
    silu_val = gate_act * sigmoid_val
    hidden = silu_val * up_act
    partial_value = jnp.sum(hidden * projected, axis=2)
    scale_col = gate_row.astype(jnp.float32)[:, :, None]
    weighted = (scale_col * hidden).astype(jnp.bfloat16)
    down_term = jnp.einsum("erf,erd->efd", weighted, rows_in, preferred_element_type=jnp.float32)
    grad_hidden = scale_col * projected
    grad_gate = (
        grad_hidden * up_act * sigmoid_val * (1.0 + gate_act * (1.0 - sigmoid_val))
    ).astype(jnp.bfloat16)
    grad_up = (grad_hidden * silu_val).astype(jnp.bfloat16)
    return (partial_value, grad_gate, grad_up, down_term)


def general_device(out_grad, routes, gate_values, gate_pre, up_pre, w_down):
    groups = lax.axis_size("expert")
    local_count = gate_pre.shape[0]
    experts = local_count * groups
    tok_count = out_grad.shape[0]
    my_rank = lax.axis_index("expert")
    flat_routes = routes.reshape(-1)
    onehot = (flat_routes[:, None] == jnp.arange(experts, dtype=jnp.int32)[None, :]).astype(
        jnp.int32
    )
    position = jnp.sum((jnp.cumsum(onehot, axis=0) - 1) * onehot, axis=1)
    own_expert = lax.dynamic_slice_in_dim(flat_routes, my_rank * tok_count * 2, tok_count * 2)
    own_position = lax.dynamic_slice_in_dim(position, my_rank * tok_count * 2, tok_count * 2)
    target = own_expert * SLOTS + own_position
    selector = target[:, None] == jnp.arange(experts * SLOTS, dtype=jnp.int32)[None, :]
    picker = selector.astype(jnp.bfloat16).T
    pair_rows = jnp.repeat(out_grad, 2, axis=0)
    send_rows = (
        jnp.dot(picker, pair_rows, preferred_element_type=jnp.float32)
        .astype(jnp.bfloat16)
        .reshape(experts, SLOTS, -1)
    )
    send_gates = (
        jnp.dot(picker, gate_values.reshape(-1, 1), preferred_element_type=jnp.float32)
        .astype(jnp.bfloat16)
        .reshape(experts, SLOTS)
    )
    got_rows, got_gates = (
        lax.all_to_all(send_rows, "expert", split_axis=0, concat_axis=0, tiled=True),
        lax.all_to_all(send_gates, "expert", split_axis=0, concat_axis=0, tiled=True),
    )
    dispatched = jnp.sum(
        got_rows.reshape(groups, local_count, SLOTS, -1).astype(jnp.float32), axis=0
    ).astype(jnp.bfloat16)
    slot_gate = jnp.sum(
        got_gates.reshape(groups, local_count, SLOTS).astype(jnp.float32), axis=0
    ).astype(jnp.bfloat16)
    all_rows, all_gates = (
        lax.all_gather(dispatched, "dp", axis=1, tiled=True),
        lax.all_gather(slot_gate, "dp", axis=1, tiled=True),
    )
    partial_value, grad_gate_pre, grad_up_pre, down_sum = expert_terms(
        gate_pre, up_pre, w_down, all_rows, all_gates
    )
    grad_down = down_sum.astype(jnp.bfloat16)
    own_sums = lax.psum_scatter(partial_value, "dp", scatter_dimension=1, tiled=True)
    score_table = lax.all_gather(own_sums, "expert", axis=0, tiled=True)
    picked = jnp.sum(jnp.where(selector, score_table.reshape(1, -1), 0.0), axis=1)
    grad_gates = picked.reshape(tok_count, 2)
    return (grad_gates, grad_gate_pre, grad_up_pre, grad_down)


LANES = 128
CORES = 2
PAD = 4
MESH = pl.DeviceIdType.MESH
BF16 = jnp.bfloat16
F32 = jnp.float32


def pow2(n):
    return n & (n - 1) == 0


def far_first(n):
    return sorted(range(1, n), reverse=True)


def fused_fits(n_dp, groups, tokens, width, local, rows, hidden):
    return (
        n_dp % CORES == 0
        and n_dp > CORES
        and groups > 1
        and pow2(groups)
        and pow2(n_dp)
        and local * PAD == 8
        and rows == n_dp * SLOTS
        and n_dp * 8 <= LANES
        and groups * tokens <= LANES
        and width % (4 * LANES) == 0
        and hidden % 512 == 0
        and n_dp * groups <= 64
        and local * hidden * width * 2 <= 26 << 20
    )


def gather_project(
    n_dp, groups, local, rows, block, pieces, early, flipped,
    grad, routes, gates, gate_pre, up_pre, weights,
    rows_out, turned_out, grad_gate_out, grad_up_out, sums_out,
    held, tokens_in, gates_in, routes_in, gate_in, up_in,
    table, high, totals, flips, silu_kept, slope_kept, turned_kept,
    sums_own, sums_all,
    load_sem, in_sem, send_z, recv_z, send_g, recv_g, send_c, recv_c, send_p, recv_p,
    send_s, recv_s,
):
    me_dp, me_z = lax.axis_index("dp"), lax.axis_index("expert")
    total = n_dp * groups
    me = me_dp * groups + me_z
    chips = n_dp // CORES
    chip, core = me_dp // CORES, lax.rem(me_dp, CORES)
    partner = chip * CORES + (1 - core)
    tokens, width = grad.shape
    hidden = held.shape[1]
    per = hidden // block
    steps = local * per
    half = width // 2
    full = n_dp * 8
    span = tokens * groups

    barrier = pltpu.get_barrier_semaphore()
    peers = [(me_dp, me_z ^ dz) for dz in far_first(groups)]
    peers += [((chip ^ dc) * CORES + core, me_z) for dc in far_first(chips)]
    peers += [(partner, me_z)]
    for peer in peers:
        pl.semaphore_signal(barrier, inc=1, device_id=peer, device_id_type=MESH)

    def local_copy(src, dst, at):
        copy = pltpu.make_async_copy(src, dst, in_sem.at[at])
        copy.start()
        return copy

    own_rows = local_copy(grad, tokens_in.at[me_z], 0)
    own_gates = local_copy(gates, gates_in.at[me_z], 1)
    own_routes = local_copy(routes, routes_in, 2)
    own_pre = local_copy(gate_pre, gate_in, 3)
    own_up = local_copy(up_pre, up_in, 4)

    def weight_copy(i):
        e, b = i // per, lax.rem(i, per)
        where = pl.ds(b * block, block)
        return pltpu.make_async_copy(weights.at[e, where], held.at[e, where], load_sem.at[i])

    own_routes.wait()
    first, second = routes_in[0:1, :], routes_in[1:2, :]
    row8 = lax.broadcasted_iota(jnp.int32, (8, 1), 0)
    lane8 = lax.broadcasted_iota(jnp.int32, (1, span), 1)
    expert_of = me_z * local + row8 // PAD
    slot_of = lax.rem(row8, PAD)
    by_choice = [(route == expert_of) for route in (first, second)]
    named = jnp.where(by_choice[0] | by_choice[1], 1, 0)
    before = jnp.zeros((8, span), jnp.int32)
    for t in range(span - 1):
        before = before + jnp.where(lane8 > t, named[:, t : t + 1], 0)
    fills = (before == slot_of) & (named > 0)
    select = jnp.where(fills, 1.0, 0.0)
    select_by = [jnp.where(fills & choice, 1.0, 0.0) for choice in by_choice]

    own_rows.wait()
    own_gates.wait()
    weight_copy(0).start()
    own_pre.wait()
    own_up.wait()
    for i in range(1, steps):
        weight_copy(i).start()

    pl.semaphore_wait(barrier, len(peers))
    stage_one = []
    for dz in far_first(groups):
        peer = (me_dp, me_z ^ dz)
        for ref, s_sem, r_sem in ((tokens_in, send_z, recv_z), (gates_in, send_g, recv_g)):
            copy = pltpu.make_async_remote_copy(
                src_ref=ref.at[me_z], dst_ref=ref.at[me_z],
                send_sem=s_sem.at[dz], recv_sem=r_sem.at[dz],
                device_id=peer, device_id_type=MESH,
            )
            copy.start()
            stage_one.append(copy)

    wide_row = lax.broadcasted_iota(jnp.int32, (full, 1), 0)
    pair_row = lax.broadcasted_iota(jnp.int32, (1, rows), 1)
    spot = (wide_row // 8) * SLOTS + lax.rem(wide_row, PAD)
    real = lax.rem(wide_row, PAD) < SLOTS
    spread = []
    for e in range(local):
        mine = real & (lax.rem(wide_row, 8) // PAD == e)
        spread.append(jnp.where(mine & (spot == pair_row), 1.0, 0.0))
    flip_row = lax.broadcasted_iota(jnp.int32, (rows, 1), 0)
    flip_col = lax.broadcasted_iota(jnp.int32, (1, full), 1)
    flip_spot = (flip_col // 8) * SLOTS + lax.rem(flip_col, PAD)
    flip_real = lax.rem(flip_col, PAD) < SLOTS
    unspread = []
    for e in range(local):
        mine = flip_real & (lax.rem(flip_col, 8) // PAD == e)
        unspread.append(jnp.where(mine & (flip_spot == flip_row), 1.0, 0.0).astype(BF16))

    owner = lax.rem(wide_row, 8) // PAD
    for c in range(0, hidden, 512):
        cols = slice(c, c + 512)
        gate_act = jnp.zeros((full, 512), F32)
        up_act = jnp.zeros((full, 512), F32)
        for e in range(local):
            pick = spread[e].astype(BF16)
            gate_act += jnp.dot(pick, gate_in[e, :, cols], preferred_element_type=F32)
            up_act += jnp.dot(pick, up_in[e, :, cols], preferred_element_type=F32)
        sigmoid_val = jax.nn.sigmoid(gate_act)
        silu_val = gate_act * sigmoid_val
        act = silu_val * up_act
        silu_kept[:, cols] = silu_val
        slope_kept[:, cols] = up_act * sigmoid_val * (1.0 + gate_act * (1.0 - sigmoid_val))
        turned_kept[cols, :] = act.T
        for e in range(local):
            part = jnp.where(owner == e, act, 0.0)
            top = part.astype(BF16)
            rest = (part - top.astype(F32)).astype(BF16)
            for b in range(512 // block):
                at = slice(b * block, (b + 1) * block)
                high[e * per + c // block + b, :full] = top[:, at]
                high[e * per + c // block + b, full:] = rest[:, at]

    eye_row = lax.broadcasted_iota(jnp.int32, (256, 256), 0)
    eye_col = lax.broadcasted_iota(jnp.int32, (256, 256), 1)
    eye = jnp.where(eye_row == eye_col, 1.0, 0.0).astype(BF16)
    by_product = (width // 1024,)

    def forward_step(i, flip):
        e, b = i // per, lax.rem(i, per)
        weight_copy(i).wait()
        left = high[i]
        for n in range(0, width, 512):
            right = held[e, pl.ds(pl.multiple_of(b * block, block), block), n : n + 512]
            totals[:, n : n + 512] += jnp.dot(left, right, preferred_element_type=F32)
            if flip and n // 512 in by_product:
                for q in range(0, 512, 256):
                    flips[i, n + q : n + q + 256, :] = lax.dot_general(
                        eye, right[:, q : q + 256], (((1,), (1,)), ((), ())),
                        preferred_element_type=F32,
                    ).astype(BF16)
            elif flip:
                flips[i, n : n + 512, :] = right.T

    def forward_steps(low, top):
        def body(flip, i, carry):
            forward_step(i, flip)
            return carry

        middle = min(max(low, flipped), top)
        if middle > low:
            lax.fori_loop(low, middle, functools.partial(body, True), 0)
        if top > middle:
            lax.fori_loop(middle, top, functools.partial(body, False), 0)

    totals[...] = jnp.zeros_like(totals)
    forward_steps(0, early[0])

    for copy in stage_one:
        copy.wait_recv()
    slots = jnp.zeros((8, width), F32)
    gate = jnp.zeros((8, 1), F32)
    for z in range(groups):
        got = tokens_in[z].astype(F32)
        got_gate = gates_in[z].astype(F32)
        for t in range(tokens):
            at = z * tokens + t
            slots = slots + select[:, at : at + 1] * got[t : t + 1, :]
            for k in range(2):
                gate = gate + select_by[k][:, at : at + 1] * got_gate[t : t + 1, k : k + 1]
    gate_wide = jnp.broadcast_to(gate, (8, LANES))
    base = pl.multiple_of(me_dp * 16, 16)
    table[pl.ds(base, 16), :half] = jnp.concatenate(
        [slots[:, :half], slots[:, half:]], axis=0
    ).astype(BF16)
    table[pl.ds(base, 16), half:] = jnp.concatenate([gate_wide, gate_wide], axis=0).astype(BF16)

    def block_copy(dp_index, target, piece, s_sem, r_sem):
        where = table.at[pl.ds(dp_index * 16, 16), pl.ds(pieces[piece], pieces[piece + 1] - pieces[piece])]
        copy = pltpu.make_async_remote_copy(
            src_ref=where, dst_ref=where, send_sem=s_sem, recv_sem=r_sem,
            device_id=(target, me_z), device_id_type=MESH,
        )
        copy.start()
        return copy

    count = len(pieces) - 1
    stage_two = {}
    stage_three = {}
    for p in range(count):
        for dc in far_first(chips):
            target = (chip ^ dc) * CORES + core
            stage_two[p, dc] = block_copy(me_dp, target, p, send_c.at[p, dc], recv_c.at[p, dc])
        stage_three[p, 0] = block_copy(me_dp, partner, p, send_p.at[p, 0], recv_p.at[p, 0])

    forward_steps(early[0], early[1])

    for p in range(count):
        for dc in range(1, chips):
            stage_two[p, dc].wait_recv()
            source = (chip ^ dc) * CORES + core
            stage_three[p, dc] = block_copy(source, partner, p, send_p.at[p, dc], recv_p.at[p, dc])

    forward_steps(early[1], steps)

    for n in range(0, width, 512):
        totals[:full, n : n + 512] += totals[full:, n : n + 512]

    for copy in stage_three.values():
        copy.wait_recv()

    part = jnp.zeros((full, LANES), F32)
    for h in range(2):
        for n in range(0, half, 512):
            got = table[:, n : n + 512].astype(F32).reshape(n_dp, 16, 512)
            got = got[:, h * 8 : h * 8 + 8].reshape(full, 512)
            at = slice(h * half + n, h * half + n + 512)
            rows_out[:, at] = got.astype(BF16)
            term = got * totals[:full, at]
            for q in range(0, 512, LANES):
                part = part + term[:, q : q + LANES]
    part = jnp.sum(part, axis=1, keepdims=True)
    lane = lax.broadcasted_iota(jnp.int32, (full, LANES), 1)
    sums = jnp.sum(jnp.where(lane == wide_row, part, 0.0), axis=0, keepdims=True)
    sums_own[...] = sums
    sums_all[me] = sums
    last = []
    offsets = [(dp, z) for z in range(groups) for dp in range(n_dp)][1:]
    for off, (dp, z) in sorted(enumerate(offsets, 1), reverse=True):
        copy = pltpu.make_async_remote_copy(
            src_ref=sums_own, dst_ref=sums_all.at[me],
            send_sem=send_s.at[off], recv_sem=recv_s.at[off],
            device_id=(me_dp ^ dp, me_z ^ z), device_id_type=MESH,
        )
        copy.start()
        last.append(copy)

    scale = table[:, half:].astype(F32).reshape(n_dp, 16, LANES)[:, :8].reshape(full, LANES)
    scale_row = scale.T[0:1, :]
    scale_col = scale[:, 0:1]
    col = lax.broadcasted_iota(jnp.int32, (1, full), 1)
    for e in range(local):
        factor = jnp.where(lax.rem(col, 8) // PAD == e, scale_row, 0.0)
        turned_out[e] = (turned_kept[...] * factor).astype(BF16)
    for i in range(flipped, steps):
        e, b = divmod(i, per)
        for n in range(0, width, 512):
            flips[i, n : n + 512, :] = held[e, b * block : (b + 1) * block, n : n + 512].T
    for c in range(0, hidden, 512):
        cols = slice(c, c + 512)
        both = []
        for e in range(local):
            both.append(
                jnp.dot(rows_out[...], flips[e * per + c // block], preferred_element_type=F32)
            )
        proj = both[0]
        for e in range(1, local):
            proj = jnp.where(owner == e, both[e], proj)
        grad_hidden = scale_col * proj
        gate_grad = (grad_hidden * slope_kept[:, cols]).astype(BF16)
        up_grad = (grad_hidden * silu_kept[:, cols]).astype(BF16)
        for e in range(local):
            for ref, value in ((grad_gate_out, gate_grad), (grad_up_out, up_grad)):
                ref[e, :, cols] = jnp.dot(
                    unspread[e], value, preferred_element_type=F32
                ).astype(BF16)

    out_row = lax.broadcasted_iota(jnp.int32, sums_out.shape, 0)
    out_col = lax.broadcasted_iota(jnp.int32, sums_out.shape, 1)
    spots = lax.broadcasted_iota(jnp.int32, (1, LANES), 1)
    masks = {}
    for k, route in enumerate((first, second)):
        ahead = jnp.zeros((1, span), jnp.int32)
        for t in range(span - 1):
            same = (first[:, t : t + 1] == route) | (second[:, t : t + 1] == route)
            ahead = ahead + jnp.where((lane8 > t) & same, 1, 0)
        for t in range(tokens):
            here = lane8 == me_z * tokens + t
            expert = jnp.sum(jnp.where(here, route, 0), axis=1, keepdims=True)
            place = jnp.sum(jnp.where(here, ahead, 0), axis=1, keepdims=True)
            for z in range(groups):
                offset = expert - z * local
                code = jnp.where(
                    (offset >= 0) & (offset < local), me_dp * 8 + offset * PAD + place, -1
                )
                masks[t, k, z] = jnp.where(spots == code, 1.0, 0.0)
    for copy in last:
        copy.wait_recv()
    sums_by = []
    for z in range(groups):
        acc = sums_all[z]
        for d in range(1, n_dp):
            acc = acc + sums_all[d * groups + z]
        sums_by.append(acc)
    result = jnp.zeros(sums_out.shape, F32)
    for t in range(tokens):
        for k in range(2):
            value = jnp.zeros((1, LANES), F32)
            for z in range(groups):
                value = value + jnp.where(masks[t, k, z] > 0.5, sums_by[z], 0.0)
            value = jnp.sum(value, axis=1, keepdims=True)
            result = jnp.where((out_row == t) & (out_col == k), value, result)
    sums_out[...] = result
    for copy in stage_one + list(stage_two.values()) + list(stage_three.values()) + last:
        copy.wait_send()


def finish(
    block, rows_in, turned, gate_grad, up_grad, sums,
    grad_sums, grad_gate, grad_up, grad_down, made, small_sem, out_sem,
):
    local, hidden, _ = turned.shape
    width = rows_in.shape[1]
    per = hidden // block
    small = []
    for at, (src, dst) in enumerate(
        ((sums, grad_sums), (gate_grad, grad_gate), (up_grad, grad_up))
    ):
        copy = pltpu.make_async_copy(src, dst, small_sem.at[at])
        copy.start()
        small.append(copy)

    def out_copy(i):
        e, b = i // per, lax.rem(i, per)
        where = pl.ds(b * block, block)
        return pltpu.make_async_copy(made.at[e, where], grad_down.at[e, where], out_sem.at[i])

    def make(e, where):
        left = turned[e, where, :]
        for n in range(0, width, 512):
            made[e, where, n : n + 512] = jnp.dot(
                left, rows_in[:, n : n + 512], preferred_element_type=F32
            ).astype(BF16)

    def body(i, carry):
        e, b = i // per, lax.rem(i, per)
        make(e, pl.ds(pl.multiple_of(b * block, block), block))
        out_copy(i).start()
        return carry

    part = block // 2
    first = []
    for q in range(2):
        where = pl.ds(q * part, part)
        make(0, where)
        copy = pltpu.make_async_copy(
            made.at[0, where], grad_down.at[0, where], small_sem.at[3 + q]
        )
        copy.start()
        first.append(copy)
    body(1, 0)
    lax.fori_loop(2, local * per, body, 0, unroll=2)

    def drain(i, carry):
        out_copy(i).wait()
        return carry

    lax.fori_loop(1, local * per, drain, 0)
    for copy in small + first:
        copy.wait()


def fused_device(out_grad, routes, gate_values, gate_pre, up_pre, w_down):
    n_dp, groups = lax.axis_size("dp"), lax.axis_size("expert")
    tokens, width = out_grad.shape
    local, rows, hidden = gate_pre.shape
    block = 512
    total = n_dp * groups
    full = n_dp * 8
    half = width // 2
    chips = n_dp // CORES
    pieces = (0, half + LANES)
    count = len(pieces) - 1
    steps = local * hidden // block
    early = (steps // 3, steps - 1)
    flipped = steps - 3
    span = groups * tokens

    vmem = pl.BlockSpec(memory_space=pltpu.VMEM)
    hbm = pl.BlockSpec(memory_space=pltpu.HBM)
    dma = pltpu.SemaphoreType.DMA
    scratch = pltpu.VMEM
    placed = [
        pltpu.with_memory_space_constraint(ref, pltpu.HBM)
        for ref in (out_grad, routes.T, gate_values, gate_pre, up_pre, w_down)
    ]
    rows_in, turned, gate_grad, up_grad, sums = pl.pallas_call(
        functools.partial(gather_project, n_dp, groups, local, rows, block, pieces, early, flipped),
        out_shape=(
            pltpu.VMEM((full, width), BF16),
            pltpu.VMEM((local, hidden, full), BF16),
            pltpu.VMEM(gate_pre.shape, BF16),
            pltpu.VMEM(up_pre.shape, BF16),
            pltpu.VMEM((tokens, 2), F32),
        ),
        in_specs=[hbm] * 6,
        out_specs=(vmem,) * 5,
        scratch_shapes=[
            scratch((local, hidden, width), BF16),
            scratch((groups, tokens, width), BF16),
            scratch((groups, tokens, 2), BF16),
            scratch((2, span), jnp.int32),
            scratch(gate_pre.shape, BF16),
            scratch(up_pre.shape, BF16),
            scratch((n_dp * 16, half + LANES), BF16),
            scratch((steps, 2 * full, block), BF16),
            scratch((2 * full, width), F32),
            scratch((steps, width, block), BF16),
            scratch((full, hidden), F32),
            scratch((full, hidden), F32),
            scratch((hidden, full), F32),
            scratch((1, LANES), F32),
            scratch((total, 1, LANES), F32),
            dma((steps,)),
            dma((5,)),
            dma((groups,)),
            dma((groups,)),
            dma((groups,)),
            dma((groups,)),
            dma((count, chips)),
            dma((count, chips)),
            dma((count, chips)),
            dma((count, chips)),
            dma((total,)),
            dma((total,)),
        ],
        compiler_params=pltpu.CompilerParams(
            collective_id=0, has_side_effects=True, vmem_limit_bytes=59 << 20
        ),
        name="gather_project",
    )(*placed)

    piece = 256
    return pl.pallas_call(
        functools.partial(finish, piece),
        out_shape=(
            jax.ShapeDtypeStruct((tokens, 2), F32),
            jax.ShapeDtypeStruct(gate_pre.shape, BF16),
            jax.ShapeDtypeStruct(up_pre.shape, BF16),
            jax.ShapeDtypeStruct(w_down.shape, BF16),
        ),
        in_specs=[vmem] * 5,
        out_specs=(hbm,) * 4,
        scratch_shapes=[
            scratch((local, hidden, width), BF16),
            dma((5,)),
            dma((local * hidden // piece,)),
        ],
        compiler_params=pltpu.CompilerParams(vmem_limit_bytes=52 << 20),
        name="finish",
    )(rows_in, turned, gate_grad, up_grad, sums)


def per_device(out_grad, routes, gate_values, gate_pre, up_pre, w_down):
    fits = fused_fits(
        lax.axis_size("dp"), lax.axis_size("expert"), *out_grad.shape, *gate_pre.shape
    )
    chosen = fused_device if fits else general_device
    return chosen(out_grad, routes, gate_values, gate_pre, up_pre, w_down)


def solution(mesh):
    return jax.shard_map(
        per_device,
        mesh=mesh,
        in_specs=(
            P(("dp", "expert"), None),
            P("dp", None),
            P(("dp", "expert"), None),
            P("expert", None, "dp"),
            P("expert", None, "dp"),
            P("expert", "dp", None),
        ),
        out_specs=(
            P(("dp", "expert"), None),
            P("expert", None, "dp"),
            P("expert", None, "dp"),
            P("expert", "dp", None),
        ),
        check_vma=False,
    )
```
